256 devices in a mesh: space: 8 (over y_hi, x), vel: 32 (over z, y_lo, core).
Axes of the slice: x: 4, y: 4 (y_hi: 2, y_lo: 2; y = y_hi * 2 + y_lo), z: 8, core: 2. Of those that a mesh axis runs over, the one named last changes fastest.
Arguments:
- distribution: float32 [8, 16, 16, 32768], P('space', None, None, 'vel'), may hold values from 0.003 to 450, as said below
- inflow: float32 [2, 16, 16, 32768], P(None, None, None, 'vel'), may hold values from 0.3 to 3
- wall_temp: float32 [2, 16, 16], replicated, may hold values from 0.5 to 4
- face_type: int32 [2, 16, 16], replicated, may hold values from 0 to 2
Outputs:
- updated: float32 [8, 16, 16, 32768], P('space', None, None, 'vel')
- fields: float32 [8, 8, 16, 16], P(None, 'space')
The draws below stay inside these ranges and needn't reach their ends.
Inputs may be any that keep to these rules, and one draw needn't show every extreme that they name: `distribution`: every entry is positive.
All inputs are finite; a program needn't handle non-finite values.
Results may differ from the reference program's by a relative error of at most 0.0003.
Values sent between devices are 32-bit elements; how exact they have to be, the bound alone decides.
No kernel may reach another device: no remote copies, remote signals or barrier semaphores. Data moves between devices by JAX's collectives and lax.ppermute only.
A program may use at most 64 MiB of HBM per device.

```python
import math
import jax
import jax.numpy as jnp

NY = 16
NZ = 16
NVX = 32
NVY = 32
NVZ = 32
OUTER = 2
INNER = 3
NX = 8
NV = 32768
VEL_DEV = 1024
N_VEL = 32


def plume_speeds():
    velocity_total = NVX * NVY * NVZ
    velocity_index = jnp.arange(velocity_total, dtype=jnp.int32)
    halves = VEL_DEV // 2
    owner_shard = velocity_index // VEL_DEV
    within = velocity_index % VEL_DEV
    upper_half = within // halves
    ranked = owner_shard * halves + within % halves
    layer_size = NVY * NVZ
    level_x = ranked // layer_size
    remain = ranked % layer_size
    across_y = remain // NVZ
    across_z = remain % NVZ
    sign_x = 2.0 * upper_half.astype(jnp.float32) - 1.0
    speed_x = sign_x * (level_x.astype(jnp.float32) + 0.5) * (8.0 / NVX)
    speed_y = (across_y.astype(jnp.float32) + 0.5) * (8.0 / NVY) - 4.0
    speed_z = (across_z.astype(jnp.float32) + 0.5) * (8.0 / NVZ) - 4.0
    return (speed_x, speed_y, speed_z)


def gas_profile(speeds, drift, temp_cell):
    offset_x = speeds[0] - drift[0]
    offset_y = speeds[1] - drift[1]
    offset_z = speeds[2] - drift[2]
    squared = offset_x * offset_x + offset_y * offset_y + offset_z * offset_z
    return 512.0 * jnp.exp(-squared / (2.0 * temp_cell)) / (2.0 * jnp.pi * temp_cell) ** 1.5


def draw_distribution(key, part):
    speeds = plume_speeds()
    cell_shape = (NX, NY, NZ, 1)
    density_key = jax.random.fold_in(key, 21)
    core_key = jax.random.fold_in(key, 22)
    beam_key = jax.random.fold_in(key, 23)
    weight_key = jax.random.fold_in(key, 24)
    core_temp_key = jax.random.fold_in(key, 25)
    beam_temp_key = jax.random.fold_in(key, 26)
    noise_key = jax.random.fold_in(key, 27)
    particle_concentration = jnp.exp(jax.random.uniform(density_key, cell_shape, jnp.float32, jnp.log(0.3), jnp.log(3.0)))
    core_local = jax.random.uniform(core_key, (3,) + cell_shape, jnp.float32, -1.0, 1.0)
    beam_local = jax.random.uniform(beam_key, (3,) + cell_shape, jnp.float32, -1.5, 1.5)
    core_drift = [core_local[index] for index in range(3)]
    beam_drift = [core_local[index] + beam_local[index] for index in range(3)]
    beam_weight = jax.random.uniform(weight_key, cell_shape, jnp.float32, 0.1, 0.35)
    core_temp = jnp.exp(jax.random.uniform(core_temp_key, cell_shape, jnp.float32, jnp.log(0.6), jnp.log(1.5)))
    beam_temp = jnp.exp(jax.random.uniform(beam_temp_key, cell_shape, jnp.float32, jnp.log(0.6), jnp.log(1.5)))
    noise = jnp.exp(jax.random.uniform(noise_key, (NX, NY, NZ, NV), jnp.float32, jnp.log(0.5), jnp.log(2.0)))
    mixture = (1.0 - beam_weight) * gas_profile(speeds, core_drift, core_temp) + beam_weight * gas_profile(speeds, beam_drift, beam_temp)
    return particle_concentration * noise * (mixture + 0.02)


def touch_ends(drawn, key, least, largest):
    shape = drawn.shape
    spot = [jax.random.randint(jax.random.fold_in(key, axis), (), 0, shape[axis]) for axis in range(len(shape))]
    drawn = drawn.at[tuple(spot)].set(least)
    longest = shape.index(max(shape))
    spot[longest] = (spot[longest] + 1) % shape[longest]
    return drawn.at[tuple(spot)].set(largest)


def block_levels(key, shape, pieces, low, high):
    gain = 1.0
    for position, shards_of in pieces:
        steps = jax.random.uniform(jax.random.fold_in(jax.random.fold_in(key, 6), position), (shards_of,), jnp.float32, low / len(pieces), high / len(pieces))
        gain = gain * jnp.repeat(jnp.exp(steps), shape[position] // shards_of).reshape((-1,) + (1,) * (len(shape) - 1 - position))
    return gain


def setup_inputs(seed: int = 0) -> dict:
    keys = jax.random.split(jax.random.key(seed), 5)
    distribution = draw_distribution(jax.random.fold_in(keys[4], 71), 0)
    inflow = jnp.clip(jnp.exp(math.log(3.0) - 2.3025851 * jax.random.uniform(keys[1], (2, NY, NZ, NV), jnp.float32) ** block_levels(keys[1], (2, NY, NZ, NV), ((3, 32),), -0.2, 0.2)), 0.3, 3.0)
    wall_temp = jnp.clip(jnp.exp(jax.random.uniform(keys[2], (2, NY, NZ), jnp.float32, math.log(0.5), math.log(4.0))), 0.5, 4.0)
    face_type = touch_ends(jax.random.randint(keys[3], (2, NY, NZ), 0, 3), jax.random.fold_in(keys[3], 1), 0, 2).astype(jnp.int32)
    return {"distribution": distribution, "inflow": inflow, "wall_temp": wall_temp, "face_type": face_type}


box_volume = 512.0
speed_top = 4.0
courant = 0.08
impact_rate_field = 0.8
shakhov_factor = 1.0 / 3.0


def velocity_table(count_x, count_y, count_z, shards):
    velocity_total = count_x * count_y * count_z
    velocity_index = jnp.arange(velocity_total, dtype=jnp.int32)
    per_shard = velocity_total // shards
    halves = per_shard // 2
    owner_shard = velocity_index // per_shard
    within = velocity_index % per_shard
    upper_half = within // halves
    ranked = owner_shard * halves + within % halves
    layer_size = count_y * count_z
    level_x = ranked // layer_size
    remain = ranked % layer_size
    across_y = remain // count_z
    across_z = remain % count_z
    sign_x = 2.0 * upper_half.astype(jnp.float32) - 1.0
    speed_x = sign_x * (level_x.astype(jnp.float32) + 0.5) * (2.0 * speed_top / count_x)
    speed_y = (across_y.astype(jnp.float32) + 0.5) * (2.0 * speed_top / count_y) - speed_top
    speed_z = (across_z.astype(jnp.float32) + 0.5) * (2.0 * speed_top / count_z) - speed_top
    return speed_x, speed_y, speed_z


def wall_shape(wall_temp, speed_sq):
    temp_cell = wall_temp[..., None]
    return box_volume * jnp.exp(-speed_sq / (2.0 * temp_cell)) / (2.0 * jnp.pi * temp_cell) ** 1.5


def boundary_planes(edge_planes, leaving, entering, wall_profile, inflow, face_type):
    wall_planes = (leaving / entering)[..., None] * wall_profile
    face_kind = face_type[..., None]
    return jnp.where(face_kind == 0, wall_planes, jnp.where(face_kind == 1, inflow, edge_planes))


def transport(current, west_plane, east_plane, speed_x, speed_y, speed_z):
    west_cells = jnp.concatenate([west_plane[None], current[:-1]], 0)
    east_cells = jnp.concatenate([current[1:], east_plane[None]], 0)
    flux_sum = jnp.maximum(speed_x, 0.0) * (current - west_cells) + jnp.minimum(speed_x, 0.0) * (east_cells - current)
    flux_sum = flux_sum + jnp.maximum(speed_y, 0.0) * (current - jnp.roll(current, 1, 1)) + jnp.minimum(speed_y, 0.0) * (jnp.roll(current, -1, 1) - current)
    flux_sum = flux_sum + jnp.maximum(speed_z, 0.0) * (current - jnp.roll(current, 1, 2)) + jnp.minimum(speed_z, 0.0) * (jnp.roll(current, -1, 2) - current)
    return current - courant * flux_sum


def macro_fields(particle_concentration, mean_motion_first_axis, mean_motion_second_axis, mean_motion_third_axis, maxwellian_width, energy_current_first, energy_current_second, energy_current_third):
    kinetic_warmth = maxwellian_width / (3.0 * particle_concentration)
    decay_rate_toward_target = impact_rate_field * particle_concentration * jnp.exp(0.19 * jnp.log(kinetic_warmth))
    return jnp.stack([particle_concentration, mean_motion_first_axis, mean_motion_second_axis, mean_motion_third_axis, kinetic_warmth, energy_current_first, energy_current_second, energy_current_third, decay_rate_toward_target])


def shakhov(params, speed_x, speed_y, speed_z):
    particle_concentration = params[0][..., None]
    peculiar_x = speed_x - params[1][..., None]
    peculiar_y = speed_y - params[2][..., None]
    peculiar_z = speed_z - params[3][..., None]
    temp_cell = params[4][..., None]
    speed_sq = peculiar_x * peculiar_x + peculiar_y * peculiar_y + peculiar_z * peculiar_z
    maxwell = particle_concentration * box_volume * jnp.exp(-speed_sq / (2.0 * temp_cell)) / (2.0 * jnp.pi * temp_cell) ** 1.5
    heat_term = (params[5][..., None] * peculiar_x + params[6][..., None] * peculiar_y + params[7][..., None] * peculiar_z) / (5.0 * particle_concentration * temp_cell * temp_cell)
    return maxwell * (1.0 + shakhov_factor * heat_term * (speed_sq / temp_cell - 5.0))


def relaxation(read, params, speed_x, speed_y, speed_z):
    decay_rate_toward_target = params[8][..., None]
    return (read + decay_rate_toward_target * shakhov(params, speed_x, speed_y, speed_z)) / (1.0 + decay_rate_toward_target)


def central_fields(current, speed_x, speed_y, speed_z, velocity_total):
    particle_concentration = jnp.sum(current, -1) / velocity_total
    mean_motion_first_axis = jnp.sum(current * speed_x, -1) / velocity_total / particle_concentration
    mean_motion_second_axis = jnp.sum(current * speed_y, -1) / velocity_total / particle_concentration
    mean_motion_third_axis = jnp.sum(current * speed_z, -1) / velocity_total / particle_concentration
    peculiar_x = speed_x - mean_motion_first_axis[..., None]
    peculiar_y = speed_y - mean_motion_second_axis[..., None]
    peculiar_z = speed_z - mean_motion_third_axis[..., None]
    speed_sq = peculiar_x * peculiar_x + peculiar_y * peculiar_y + peculiar_z * peculiar_z
    maxwellian_width = jnp.sum(current * speed_sq, -1) / velocity_total
    energy_current_first = 0.5 * jnp.sum(current * peculiar_x * speed_sq, -1) / velocity_total
    energy_current_second = 0.5 * jnp.sum(current * peculiar_y * speed_sq, -1) / velocity_total
    energy_current_third = 0.5 * jnp.sum(current * peculiar_z * speed_sq, -1) / velocity_total
    return macro_fields(particle_concentration, mean_motion_first_axis, mean_motion_second_axis, mean_motion_third_axis, maxwellian_width, energy_current_first, energy_current_second, energy_current_third)


def reference(distribution, inflow, wall_temp, face_type):
    velocity_total = NVX * NVY * NVZ
    speed_x, speed_y, speed_z = velocity_table(NVX, NVY, NVZ, N_VEL)
    speed_sq = speed_x * speed_x + speed_y * speed_y + speed_z * speed_z
    wall_profile = wall_shape(wall_temp, speed_sq)
    outward = jnp.stack([-speed_x, speed_x])[:, None, None, :]
    entering = jnp.sum(wall_profile * jnp.maximum(-outward, 0.0), -1)
    current = distribution
    params = None
    for outer_turn in range(OUTER):
        edge_planes = jnp.stack([current[0], current[-1]])
        leaving = jnp.sum(edge_planes * jnp.maximum(outward, 0.0), -1)
        ghost_planes = boundary_planes(edge_planes, leaving, entering, wall_profile, inflow, face_type)
        read = transport(current, ghost_planes[0], ghost_planes[1], speed_x, speed_y, speed_z)
        current = read
        for inner_turn in range(INNER):
            params = central_fields(current, speed_x, speed_y, speed_z, velocity_total)
            current = relaxation(read, params, speed_x, speed_y, speed_z)
    return current, params[:8]
```

```python
import functools

import jax
import jax.numpy as jnp
import numpy as np
from jax import lax
from jax.experimental import pallas as pl
from jax.experimental.pallas import tpu as pltpu
from jax.sharding import Mesh, PartitionSpec as P


NV = 32768
CELLS = 256
HALF = 512
NK = 13
ROWS = 112
HROWS = ROWS // 2
courant = 0.08
rate_field = 0.8
box_volume = 512.0
HIGHEST = lax.Precision.HIGHEST
f32 = jnp.float32

MOMENTS = [
    [(0, 0, 0)],
    [(1, 0, 0)],
    [(0, 1, 0)],
    [(0, 0, 1)],
    [(2, 0, 0)],
    [(0, 2, 0)],
    [(0, 0, 2)],
    [(1, 1, 0)],
    [(1, 0, 1)],
    [(0, 1, 1)],
    [(3, 0, 0), (1, 2, 0), (1, 0, 2)],
    [(2, 1, 0), (0, 3, 0), (0, 1, 2)],
    [(2, 0, 1), (0, 2, 1), (0, 0, 3)],
]


def axis_tables():
    grid = (np.arange(32) + 0.5) * 0.25 - 4.0
    plus, minus = courant * np.maximum(grid, 0.0), courant * np.maximum(-grid, 0.0)
    table = np.zeros((96, 96))
    for axis in range(3):
        for power in range(4):
            for d in range(7):
                row = grid**power
                if d == 1 + 2 * axis:
                    row = row * plus
                if d == 2 + 2 * axis:
                    row = row * minus
                table[32 * axis + 8 * power + d, 32 * axis : 32 * axis + 32] = row
    walls = []
    for weight in (plus, minus):
        wall = table.copy()
        wall[:32, :32] *= weight
        walls.append(np.concatenate([table, wall]))
    return table.astype(np.float32), np.stack(walls).astype(np.float32)


TABLE, WALL_TABLES = axis_tables()


def dot(a, b):
    return lax.dot_general(a, b, (((1,), (0,)), ((), ())), precision=HIGHEST, preferred_element_type=f32)


def dot_t(a, b):
    return lax.dot_general(a, b, (((1,), (1,)), ((), ())), precision=HIGHEST, preferred_element_type=f32)


def tile4(a):
    return jnp.concatenate([a] * 4, 0)


def speed_grid():
    return (lax.broadcasted_iota(jnp.int32, (32, CELLS), 0).astype(f32) + 0.5) * 0.25 - 4.0


def lane_speeds(p, rows):
    lane = lax.broadcasted_iota(jnp.int32, (rows, HALF), 1)
    cy = ((lane // 32 + (p % 2) * 16).astype(f32) + 0.5) * 0.25 - 4.0
    cz = ((lane % 32).astype(f32) + 0.5) * 0.25 - 4.0
    return cy, cz


def speed_x(p):
    return ((p // 2).astype(f32) + 0.5) * 0.25


def to_columns(rows):
    pad = 128 - rows.shape[0]
    return jnp.transpose(jnp.concatenate([rows, jnp.zeros((pad, CELLS), f32)], 0))


def equilibrium_moments(params, table):
    n, ux, uy, uz, temp, qx, qy, qz = params
    inv = 1.0 / temp
    two_pi = 2.0 * np.pi * temp
    pref = n * box_volume / (two_pi * jnp.sqrt(two_pi))
    scale = inv * inv / (15.0 * n)
    grid = speed_grid()
    decay = tile4(-0.5 * inv)
    columns = []
    for u in (ux, uy, uz):
        w = grid - tile4(u)
        g = jnp.exp(w * w * decay)
        g1 = g * w
        g2 = g1 * w
        columns.append(jnp.concatenate([g, g1, g2, g2 * w], 1))
    sums = dot(table, jnp.concatenate(columns, 0))
    factors = []
    for axis, q in enumerate((qx, qy, qz)):
        kq = q * scale
        powers = []
        for power in range(4):
            row = 32 * axis + 8 * power
            t0, t1, t2, t3 = [sums[row : row + 8, CELLS * b : CELLS * (b + 1)] for b in range(4)]
            powers.append((t0, kq * t1, t2 * inv, kq * (t3 * inv - 5.0 * t1)))
        factors.append(powers)
    xs, ys, zs = factors
    pairs = {}

    def pair(ay, az):
        if (ay, az) not in pairs:
            y0, y1, y2, y3 = ys[ay]
            z0, z1, z2, z3 = zs[az]
            a = y0 * z0
            b = a + y3 * z0 + y0 * z3 + y1 * z2 + y2 * z1
            pairs[(ay, az)] = (a, b, y2 * z0 + y0 * z2, y1 * z0 + y0 * z1)
        return pairs[(ay, az)]

    out = []
    for terms in MOMENTS:
        total = 0.0
        for ax, ay, az in terms:
            x0, x1, x2, x3 = xs[ax]
            a, b, c, d = pair(ay, az)
            total = total + (x0 * b + x3 * a + x1 * c + x2 * d)
        out.append(pref * total)
    return out


def wall_moments(temp, tables):
    grid = speed_grid()
    g = jnp.exp(grid * grid * tile4(-0.5 / temp))
    sums = dot(tables, jnp.concatenate([g] * 3, 0))
    two_pi = 2.0 * np.pi * temp
    pref = box_volume / (two_pi * jnp.sqrt(two_pi))
    out = []
    for base in (0, 96):
        for terms in MOMENTS:
            total = 0.0
            for powers in terms:
                part = pref
                for axis in range(3):
                    row = base + 32 * axis + 8 * powers[axis]
                    part = part * sums[row : row + 8]
                total = total + part
            out.append(total)
    return out


def macro(m):
    m = [a * (1.0 / NV) for a in m]
    n = m[0]
    rn = 1.0 / n
    ux, uy, uz = m[1] * rn, m[2] * rn, m[3] * rn
    square = ux * ux + uy * uy + uz * uz
    energy = m[4] + m[5] + m[6]
    temp = (energy - n * square) * rn * (1.0 / 3.0)
    lift = 2.0 * n * square - energy
    qx = 0.5 * (m[10] + ux * lift) - (ux * m[4] + uy * m[7] + uz * m[8])
    qy = 0.5 * (m[11] + uy * lift) - (ux * m[7] + uy * m[5] + uz * m[9])
    qz = 0.5 * (m[12] + uz * lift) - (ux * m[8] + uy * m[9] + uz * m[6])
    rate = rate_field * n * jnp.exp(0.19 * jnp.log(temp))
    return (n, ux, uy, uz, temp, qx, qy, qz), rate


def spread(row):
    return jnp.broadcast_to(row, (8, CELLS))


def relax_params(m, table):
    params, rate = macro(m)
    for _ in range(2):
        s = [spread(a[:1]) for a in equilibrium_moments(params, table)]
        inv = 1.0 / (1.0 + rate)
        params, rate = macro([(a + rate * b) * inv for a, b in zip(m, s)])
    return params, rate


def setup_kernel(scal, infl, f0, f1, temp_ref, type_ref, tables, weights, pre, wall, wall_bulk, cols):
    x, p = scal[0], scal[1]
    cxd = speed_x(p)
    cy, cz = lane_speeds(p, 8)
    d = lax.broadcasted_iota(jnp.int32, (8, HALF), 0)
    upper = x == 7
    common = jnp.where(d == 0, 1.0, 0.0)
    common = jnp.where(d == 3, courant * jnp.maximum(cy, 0.0), common)
    common = jnp.where(d == 4, courant * jnp.maximum(-cy, 0.0), common)
    common = jnp.where(d == 5, courant * jnp.maximum(cz, 0.0), common)
    common = jnp.where(d == 6, courant * jnp.maximum(-cz, 0.0), common)
    for half in range(2):
        cx = cxd if half else -cxd
        multiplier = jnp.where(d == 1 + (1 - half), courant * cxd, common)
        ypow = [1.0, cy, cy * cy, cy * cy * cy]
        zpow = [1.0, cz, cz * cz, cz * cz * cz]
        xpow = [1.0, cx, cx * cx, cx * cx * cx]
        for k, terms in enumerate(MOMENTS):
            phi = 0.0
            for ax, ay, az in terms:
                phi = phi + xpow[ax] * (ypow[ay] * zpow[az])
            weights[8 * k : 8 * k + 8, HALF * half : HALF * half + HALF] = multiplier * phi
        weights[8 * NK : ROWS, HALF * half : HALF * half + HALF] = jnp.zeros((8, HALF), f32)
    side = jnp.where(upper, 0, 1)
    start = pl.multiple_of(side * HALF, HALF)
    in_rows = dot_t(weights[:, pl.ds(start, HALF)], infl[...])
    dd = lax.broadcasted_iota(jnp.int32, (ROWS, CELLS), 0)
    outgoing = jnp.where(upper, f1[...], f0[...])
    flux = dot_t(jnp.full((8, HALF), 1.0, f32), outgoing) * cxd
    edge = jnp.where(jnp.logical_or(x == 0, upper), 1.0, 0.0)
    shifted = []
    for k in range(NK):
        row = in_rows[8 * k + 1 : 8 * k + 2]
        row2 = in_rows[8 * k + 2 : 8 * k + 3]
        pick = jnp.where(upper, row2, row)
        sub = lax.broadcasted_iota(jnp.int32, (8, CELLS), 0)
        pre[8 * k : 8 * k + 8, :] = jnp.where(sub == 7, jnp.broadcast_to(pick, (8, CELLS)), 0.0) * edge
    pre[8 * NK : ROWS, :] = flux * edge
    temp = temp_ref[...]
    for k, value in enumerate(wall_moments(temp, tables[...])):
        wall[8 * k : 8 * k + 8, :] = value
    kind = type_ref[...]
    sub = lax.broadcasted_iota(jnp.int32, (8, CELLS), 0)
    rows = jnp.where(sub == 0, jnp.where(kind == 1.0, edge, 0.0), 0.0)
    rows = jnp.where(sub == 1, jnp.where(kind == 2.0, edge, 0.0), rows)
    rows = jnp.where(sub == 2, -0.5 / temp, rows)
    two_pi = 2.0 * np.pi * temp
    rows = jnp.where(sub == 3, box_volume / (two_pi * jnp.sqrt(two_pi)), rows)
    cols[...] = to_columns(rows)
    cy16, cz16 = lane_speeds(p, 16)
    speed_sq = cy16 * cy16 + cz16 * cz16 + cxd * cxd

    def step(i, carry):
        at = pl.ds(pl.multiple_of(i * 16, 16), 16)
        c = cols[at, :]
        wall_bulk[at, :] = c[:, 3:4] * jnp.exp(speed_sq * c[:, 2:3])
        return carry

    lax.fori_loop(0, 16, step, 0)


def upwind_y(p, i):
    return pl.ds(pl.multiple_of(((i + jnp.where(p % 2 == 1, 15, 1)) % 16) * 16, 16), 16)


def transport_block(value, neighbour_y, plane, p, cxd, cy, cz):
    abs_y, abs_z = courant * jnp.abs(cy), courant * jnp.abs(cz)
    centre = 1.0 - courant * cxd - abs_y - abs_z
    neighbour_z = jnp.where(cz > 0.0, pltpu.roll(value, 1, 0), pltpu.roll(value, 15, 0))
    return value * centre + (courant * cxd) * plane + abs_y * neighbour_y + abs_z * neighbour_z


def read_kernel(scal, f0, f1, h0, h1, infl, cols, weights, pre, r0, r1, keep, send):
    x, p = scal[0], scal[1]
    cxd = speed_x(p)
    cy, cz = lane_speeds(p, 16)
    low = jnp.where(x == 0, 1.0, 0.0)
    high = jnp.where(x == 7, 1.0, 0.0)

    def step(i, carry):
        at = pl.ds(pl.multiple_of(i * 16, 16), 16)
        up = upwind_y(p, i)
        c = cols[at, :]
        inflow = infl[at, :] * c[:, 0:1]
        mirror = c[:, 1:2]
        for f, h, r, side in ((f0, h0, r0, high), (f1, h1, r1, low)):
            value = f[at, :]
            plane = h[at, :] + side * (inflow + mirror * value)
            r[at, :] = transport_block(value, f[up, :], plane, p, cxd, cy, cz)
        return carry

    lax.fori_loop(0, 16, step, 0)
    rows = pre[...] + dot_t(weights[:, :HALF], r0[...]) + dot_t(weights[:, HALF:], r1[...])
    north = p % 2 == 1
    top, bottom = rows[:HROWS], rows[HROWS:]
    keep[...] = jnp.where(north, bottom, top)
    send[...] = jnp.where(north, top, bottom)


def cell_kernel(scal, mine, other, wall, type_ref, table, to_east, to_west, own, state):
    x, p = scal[0], scal[1]
    upper = x == 7
    edge = jnp.where(jnp.logical_or(x == 0, upper), 1.0, 0.0)
    north = p % 2 == 1
    a, b = mine[...], other[...]
    rows = jnp.concatenate([jnp.where(north, b, a), jnp.where(north, a, b)], 0)
    m = [rows[8 * k : 8 * k + 8] for k in range(NK)]
    plain = [wall[8 * k : 8 * k + 8, :] for k in range(NK)]
    kind = type_ref[...]
    is_wall = jnp.where(kind == 0.0, edge, 0.0)
    is_in = jnp.where(kind == 1.0, edge, 0.0)
    is_out = jnp.where(kind == 2.0, edge, 0.0)

    def inward(v):
        return spread(jnp.where(upper, v[2:3], v[1:2]))

    def outward(v):
        return spread(jnp.where(upper, v[1:2], v[2:3]))

    entering = inward(plain[0]) * (1.0 / courant)
    amp = is_wall * spread(rows[8 * NK : 8 * NK + 1]) / entering
    inflow = [spread(v[7:8]) for v in m]
    m = [v + amp * wall[8 * (NK + k) : 8 * (NK + k) + 8, :] for k, v in enumerate(m)]
    params, rate = relax_params([spread(v[:1]) for v in m], table[...])
    s = equilibrium_moments(params, table[...])
    inv = 1.0 / (1.0 + rate)
    m = [(v + rate * w) * inv for v, w in zip(m, s)]
    amp2 = is_wall * outward(m[0]) * (1.0 / courant) / entering
    sub = lax.broadcasted_iota(jnp.int32, (8, CELLS), 0)
    lane = lax.broadcasted_iota(jnp.int32, (8, CELLS), 1)
    first, last = lane % 16 == 0, lane % 16 == 15
    for k in range(NK):
        v = m[k]
        z_up = jnp.where(first, pltpu.roll(v, CELLS - 15, 1), pltpu.roll(v, 1, 1))
        z_down = jnp.where(last, pltpu.roll(v, 15, 1), pltpu.roll(v, CELLS - 1, 1))
        total = jnp.where(sub == 0, v, jnp.where(sub == 7, 0.0, -v))
        total = total + jnp.where(sub == 3, pltpu.roll(v, 16, 1), 0.0)
        total = total + jnp.where(sub == 4, pltpu.roll(v, CELLS - 16, 1), 0.0)
        total = total + jnp.where(sub == 5, z_up, 0.0) + jnp.where(sub == 6, z_down, 0.0)
        ghost = amp2 * inward(plain[k]) + is_in * inflow[k] + is_out * inward(v)
        own[k : k + 1, :] = jnp.sum(total, 0, keepdims=True) + ghost[:1]
        to_east[k : k + 1, :] = v[1:2]
        to_west[k : k + 1, :] = v[2:3]
    own[NK:16, :] = jnp.zeros((3, CELLS), f32)
    extra = list(params) + [rate, amp]
    for k, v in enumerate(extra):
        to_east[NK + k : NK + k + 1, :] = v[:1]
        to_west[NK + k : NK + k + 1, :] = v[:1]
        state[k : k + 1, :] = v[:1]
    to_east[23:24, :] = jnp.zeros((1, CELLS), f32)
    to_west[23:24, :] = jnp.zeros((1, CELLS), f32)
    state[10:11, :] = amp2[:1]
    state[11:16, :] = jnp.zeros((5, CELLS), f32)


NCOL = 12


def bulk_rows(params, rate, wall):
    n, ux, uy, uz, temp, qx, qy, qz = params
    inv = 1.0 / temp
    two_pi = 2.0 * np.pi * temp
    share = 1.0 / (1.0 + rate)
    scale = inv * inv / (15.0 * n)
    return [
        ux,
        uy,
        uz,
        -0.5 * inv,
        inv,
        qx * scale,
        qy * scale,
        qz * scale,
        rate * share * n * box_volume / (two_pi * jnp.sqrt(two_pi)),
        share,
        wall,
    ]


def relaxed(value, c, base, cx, cy, cz):
    def col(j):
        return c[:, base + j : base + j + 1]

    wx = cx - col(0)
    wy = cy - col(1)
    wz = cz - col(2)
    square = wx * wx + wy * wy + wz * wz
    heat = col(5) * wx + col(6) * wy + col(7) * wz
    shape = 1.0 + heat * (square * col(4) - 5.0)
    return value * col(9) + col(8) * jnp.exp(square * col(3)) * shape


def final_kernel(
    scal, r0, r1, h0, h1, from_west, from_east, own, state, wall_bulk, infl, cols, table, out, fields, c1, planes, work
):
    x, p = scal[0], scal[1]
    cxd = speed_x(p)
    cy, cz = lane_speeds(p, 16)
    west, east = from_west[...], from_east[...]
    lone = x == 0
    lone_e = x == 7
    st = state[...]
    m = [spread(own[k : k + 1, :] + west[k : k + 1] + east[k : k + 1]) for k in range(NK)]
    params, rate = relax_params(m, table[...])
    for k in range(8):
        fields[k : k + 1, :] = params[k][:1]
    low, high = jnp.where(x == 0, 1.0, 0.0), jnp.where(x == 7, 1.0, 0.0)
    near_low, near_high = jnp.where(x == 1, 1.0, 0.0), jnp.where(x == 6, 1.0, 0.0)
    wall_scale = courant * cxd

    def single(source, base):
        return [source[base + k : base + k + 1] for k in range(8)], source[base + 8 : base + 9], source[base + 9 : base + 10]

    mine, rate1, amp = single(st, 0)
    west = jnp.concatenate([west[:NK], jnp.where(lone, st[:10], west[NK : NK + 10])], 0)
    east = jnp.concatenate([east[:NK], jnp.where(lone_e, st[:10], east[NK : NK + 10])], 0)
    wp, wr, wa = single(west, NK)
    ep, er, ea = single(east, NK)
    rows = []
    rows += bulk_rows(mine, rate1, amp * wall_scale) + [st[10:11]]
    rows += bulk_rows(ep, er, ea * wall_scale * near_high) + [jnp.zeros((1, CELLS), f32)]
    rows += bulk_rows(wp, wr, wa * wall_scale * near_low) + [jnp.zeros((1, CELLS), f32)]
    rows += bulk_rows([v[:1] for v in params], rate[:1], jnp.zeros((1, CELLS), f32)) + [jnp.zeros((1, CELLS), f32)]
    work[...] = to_columns(jnp.concatenate(rows, 0))
    in_low, in_high = 1.0 - low, 1.0 - high

    def first(i, carry):
        at = pl.ds(pl.multiple_of(i * 16, 16), 16)
        c = work[at, :]
        k = cols[at, :]
        w = wall_bulk[at, :]
        inflow = infl[at, :] * k[:, 0:1] + c[:, 11:12] * w
        mirror = k[:, 1:2]
        for half, r, h, edge, inner, base in ((0, r0, h0, high, in_high, NCOL), (1, r1, h1, low, in_low, 2 * NCOL)):
            cx = cxd if half else -cxd
            lanes = slice(HALF * half, HALF * half + HALF)
            value = relaxed(r[at, :] + (edge * c[:, 10:11]) * w, c, 0, cx, cy, cz)
            halo = relaxed(h[at, :] + c[:, base + 10 : base + 11] * w, c, base, cx, cy, cz)
            c1[at, lanes] = value
            planes[at, lanes] = inner * halo + edge * (inflow + mirror * value)
        return carry

    lax.fori_loop(0, 16, first, 0)

    def second(i, carry):
        at = pl.ds(pl.multiple_of(i * 16, 16), 16)
        up = upwind_y(p, i)
        c = work[at, :]
        for half in range(2):
            cx = cxd if half else -cxd
            lanes = slice(HALF * half, HALF * half + HALF)
            read = transport_block(c1[at, lanes], c1[up, lanes], planes[at, lanes], p, cxd, cy, cz)
            out[at, lanes] = relaxed(read, c, 3 * NCOL, cx, cy, cz)
        return carry

    lax.fori_loop(0, 16, second, 0)


VMEM = pl.BlockSpec(memory_space=pltpu.VMEM)
SMEM = pl.BlockSpec(memory_space=pltpu.SMEM)


def call(kernel, outs, args, scratch=(), cost=10_000_000):
    return pl.pallas_call(
        kernel,
        out_shape=[jax.ShapeDtypeStruct(s, f32) for s in outs],
        in_specs=[SMEM] + [VMEM] * (len(args) - 1),
        out_specs=[VMEM] * len(outs),
        scratch_shapes=[pltpu.VMEM(s, f32) for s in scratch],
        cost_estimate=pl.CostEstimate(flops=cost, bytes_accessed=1 << 20, transcendentals=0),
        compiler_params=pltpu.CompilerParams(vmem_limit_bytes=32 << 20),
    )(*args)


EAST = [(i, i + 1) for i in range(7)]
WEST = [(i + 1, i) for i in range(7)]
SWAP = [(0, 1), (1, 0)]


def body(distribution, inflow, wall_temp, face_type):
    x = lax.axis_index("space")
    p = lax.axis_index("z") * 4 + lax.axis_index("ylo") * 2 + lax.axis_index("core")
    scal = jnp.stack([x, p]).astype(jnp.int32)
    f = distribution.reshape(CELLS, 2 * HALF)
    f0, f1 = f[:, :HALF], f[:, HALF:]
    h0 = lax.ppermute(f0, "space", WEST)
    h1 = lax.ppermute(f1, "space", EAST)
    face = jnp.where(x >= 4, 1, 0)
    infl = lax.dynamic_slice(inflow.reshape(2, CELLS, 2 * HALF), (face, 0, HALF * (1 - face)), (1, CELLS, HALF))[0]
    temp = lax.dynamic_index_in_dim(wall_temp.reshape(2, CELLS), face, 0)
    kind = lax.dynamic_index_in_dim(face_type.reshape(2, CELLS), face, 0).astype(f32)
    temp, kind = jnp.broadcast_to(temp, (8, CELLS)), jnp.broadcast_to(kind, (8, CELLS))
    tables = lax.dynamic_index_in_dim(jnp.asarray(WALL_TABLES), face, 0, keepdims=False)
    table = jnp.asarray(TABLE)
    weights, pre, wall, wall_bulk, cols = call(
        setup_kernel,
        [(ROWS, 2 * HALF), (ROWS, CELLS), (2 * NK * 8, CELLS), (CELLS, HALF), (CELLS, 128)],
        [scal, infl, f0, f1, temp, kind, tables],
    )
    r0, r1, keep, send = call(
        read_kernel,
        [(CELLS, HALF), (CELLS, HALF), (HROWS, CELLS), (HROWS, CELLS)],
        [scal, f0, f1, h0, h1, infl, cols, weights, pre],
    )
    g0 = lax.ppermute(r0, "space", WEST)
    g1 = lax.ppermute(r1, "space", EAST)
    part = keep + lax.ppermute(send, "core", SWAP)
    part = part + lax.ppermute(part, "ylo", SWAP)
    part = jnp.sum(lax.all_to_all(jnp.broadcast_to(part[None], (8, HROWS, CELLS)), "z", 0, 0), 0)
    other = lax.ppermute(part, "core", SWAP)
    to_east, to_west, own, state = call(
        cell_kernel,
        [(24, CELLS), (24, CELLS), (16, CELLS), (16, CELLS)],
        [scal, part, other, wall, kind, table],
    )
    from_west = lax.ppermute(to_east, "space", EAST)
    from_east = lax.ppermute(to_west, "space", WEST)
    out, fields = call(
        final_kernel,
        [(CELLS, 2 * HALF), (8, CELLS)],
        [scal, r0, r1, g0, g1, from_west, from_east, own, state, wall_bulk, infl, cols, table],
        [(CELLS, 2 * HALF), (CELLS, 2 * HALF), (CELLS, 128)],
    )
    return out.reshape(1, 16, 16, 2 * HALF), fields.reshape(8, 1, 16, 16)


def solution(mesh):
    split = Mesh(mesh.devices.reshape(8, 8, 2, 2), ("space", "z", "ylo", "core"))
    vel = ("z", "ylo", "core")
    in_specs = (P("space", None, None, vel), P(None, None, None, vel), P(), P())
    out_specs = (P("space", None, None, vel), P(None, "space", None, None))
    return jax.shard_map(body, mesh=split, in_specs=in_specs, out_specs=out_specs, check_vma=False)
```

```python
import jax
import jax.numpy as jnp
import numpy as np
from jax import lax
from jax.experimental import pallas as pl
from jax.experimental.pallas import tpu as pltpu
from jax.sharding import Mesh, PartitionSpec as P


NV = 32768
CELLS = 256
HALF = 512
NK = 13
ROWS = 112
HROWS = ROWS // 2
courant = 0.08
rate_field = 0.8
box_volume = 512.0
HIGHEST = lax.Precision.HIGHEST
f32 = jnp.float32

MOMENTS = [
    [(0, 0, 0)],
    [(1, 0, 0)],
    [(0, 1, 0)],
    [(0, 0, 1)],
    [(2, 0, 0)],
    [(0, 2, 0)],
    [(0, 0, 2)],
    [(1, 1, 0)],
    [(1, 0, 1)],
    [(0, 1, 1)],
    [(3, 0, 0), (1, 2, 0), (1, 0, 2)],
    [(2, 1, 0), (0, 3, 0), (0, 1, 2)],
    [(2, 0, 1), (0, 2, 1), (0, 0, 3)],
]


def axis_tables():
    grid = (np.arange(32) + 0.5) * 0.25 - 4.0
    plus, minus = courant * np.maximum(grid, 0.0), courant * np.maximum(-grid, 0.0)
    table = np.zeros((96, 96))
    for axis in range(3):
        for power in range(4):
            for d in range(7):
                row = grid**power
                if d == 1 + 2 * axis:
                    row = row * plus
                if d == 2 + 2 * axis:
                    row = row * minus
                table[32 * axis + 8 * power + d, 32 * axis : 32 * axis + 32] = row
    walls = []
    for weight in (plus, minus):
        wall = table.copy()
        wall[:32, :32] *= weight
        walls.append(np.concatenate([table, wall]))
    return table.astype(np.float32), np.stack(walls).astype(np.float32)


TABLE, WALL_TABLES = axis_tables()


def dot(a, b):
    return lax.dot_general(a, b, (((1,), (0,)), ((), ())), precision=HIGHEST, preferred_element_type=f32)


def dot_t(a, b):
    return lax.dot_general(a, b, (((1,), (1,)), ((), ())), precision=HIGHEST, preferred_element_type=f32)


def tile4(a):
    return jnp.concatenate([a] * 4, 0)


def speed_grid():
    return (lax.broadcasted_iota(jnp.int32, (32, CELLS), 0).astype(f32) + 0.5) * 0.25 - 4.0


def lane_speeds(p, rows):
    lane = lax.broadcasted_iota(jnp.int32, (rows, HALF), 1)
    cy = ((lane // 32 + (p % 2) * 16).astype(f32) + 0.5) * 0.25 - 4.0
    cz = ((lane % 32).astype(f32) + 0.5) * 0.25 - 4.0
    return cy, cz


def speed_x(p):
    return ((p // 2).astype(f32) + 0.5) * 0.25


def to_columns(rows):
    pad = 128 - rows.shape[0]
    return jnp.transpose(jnp.concatenate([rows, jnp.zeros((pad, CELLS), f32)], 0))


def equilibrium_moments(params, table):
    n, ux, uy, uz, temp, qx, qy, qz = params
    inv = 1.0 / temp
    two_pi = 2.0 * np.pi * temp
    pref = n * box_volume / (two_pi * jnp.sqrt(two_pi))
    scale = inv * inv / (15.0 * n)
    grid = speed_grid()
    decay = tile4(-0.5 * inv)
    columns = []
    for u in (ux, uy, uz):
        w = grid - tile4(u)
        g = jnp.exp(w * w * decay)
        g1 = g * w
        g2 = g1 * w
        columns.append(jnp.concatenate([g, g1, g2, g2 * w], 1))
    sums = dot(table, jnp.concatenate(columns, 0))
    factors = []
    for axis, q in enumerate((qx, qy, qz)):
        kq = q * scale
        powers = []
        for power in range(4):
            row = 32 * axis + 8 * power
            t0, t1, t2, t3 = [sums[row : row + 8, CELLS * b : CELLS * (b + 1)] for b in range(4)]
            powers.append((t0, kq * t1, t2 * inv, kq * (t3 * inv - 5.0 * t1)))
        factors.append(powers)
    xs, ys, zs = factors
    pairs = {}

    def pair(ay, az):
        if (ay, az) not in pairs:
            y0, y1, y2, y3 = ys[ay]
            z0, z1, z2, z3 = zs[az]
            a = y0 * z0
            b = a + y3 * z0 + y0 * z3 + y1 * z2 + y2 * z1
            pairs[(ay, az)] = (a, b, y2 * z0 + y0 * z2, y1 * z0 + y0 * z1)
        return pairs[(ay, az)]

    out = []
    for terms in MOMENTS:
        total = 0.0
        for ax, ay, az in terms:
            x0, x1, x2, x3 = xs[ax]
            a, b, c, d = pair(ay, az)
            total = total + (x0 * b + x3 * a + x1 * c + x2 * d)
        out.append(pref * total)
    return out


def wall_moments(temp, tables):
    grid = speed_grid()
    g = jnp.exp(grid * grid * tile4(-0.5 / temp))
    sums = dot(tables, jnp.concatenate([g] * 3, 0))
    two_pi = 2.0 * np.pi * temp
    pref = box_volume / (two_pi * jnp.sqrt(two_pi))
    out = []
    for base in (0, 96):
        for terms in MOMENTS:
            total = 0.0
            for powers in terms:
                part = pref
                for axis in range(3):
                    row = base + 32 * axis + 8 * powers[axis]
                    part = part * sums[row : row + 8]
                total = total + part
            out.append(total)
    return out


def macro(m):
    m = [a * (1.0 / NV) for a in m]
    n = m[0]
    rn = 1.0 / n
    ux, uy, uz = m[1] * rn, m[2] * rn, m[3] * rn
    square = ux * ux + uy * uy + uz * uz
    energy = m[4] + m[5] + m[6]
    temp = (energy - n * square) * rn * (1.0 / 3.0)
    lift = 2.0 * n * square - energy
    qx = 0.5 * (m[10] + ux * lift) - (ux * m[4] + uy * m[7] + uz * m[8])
    qy = 0.5 * (m[11] + uy * lift) - (ux * m[7] + uy * m[5] + uz * m[9])
    qz = 0.5 * (m[12] + uz * lift) - (ux * m[8] + uy * m[9] + uz * m[6])
    rate = rate_field * n * jnp.exp(0.19 * jnp.log(temp))
    return (n, ux, uy, uz, temp, qx, qy, qz), rate


def spread(row):
    return jnp.broadcast_to(row, (8, CELLS))


def relax_params(m, table):
    params, rate = macro(m)
    for _ in range(2):
        s = [spread(a[:1]) for a in equilibrium_moments(params, table)]
        inv = 1.0 / (1.0 + rate)
        params, rate = macro([(a + rate * b) * inv for a, b in zip(m, s)])
    return params, rate


def here():
    x = lax.axis_index("space")
    p = lax.axis_index("z") * 4 + lax.axis_index("ylo") * 2 + lax.axis_index("core")
    return x, p


def half_start(index):
    return pl.multiple_of(index * HALF, HALF)


def split_kernel(f, fa, fb, sems):
    x, _ = here()
    odd = x % 2
    first = pltpu.make_async_copy(f.at[:, pl.ds(half_start(1 - odd), HALF)], fa, sems.at[0])
    second = pltpu.make_async_copy(f.at[:, pl.ds(half_start(odd), HALF)], fb, sems.at[1])
    first.start()
    second.start()
    first.wait()
    second.wait()


def setup_kernel(inflow, fb, temp_ref, type_ref, tables, infl, wa, wb, pre, wall, wall_bulk, cols, sems):
    x, p = here()
    odd = x % 2
    face = jnp.where(x >= 4, 1, 0)
    copy = pltpu.make_async_copy(inflow.at[face, :, pl.ds(half_start(1 - odd), HALF)], infl, sems.at[0])
    copy.start()
    cxd = speed_x(p)
    cy, cz = lane_speeds(p, 8)
    d = lax.broadcasted_iota(jnp.int32, (8, HALF), 0)
    common = jnp.where(d == 0, 1.0, 0.0)
    common = jnp.where(d == 3, courant * jnp.maximum(cy, 0.0), common)
    common = jnp.where(d == 4, courant * jnp.maximum(-cy, 0.0), common)
    common = jnp.where(d == 5, courant * jnp.maximum(cz, 0.0), common)
    common = jnp.where(d == 6, courant * jnp.maximum(-cz, 0.0), common)
    sign_a = jnp.where(odd == 0, 1.0, -1.0)
    for w, sign, row in ((wa, sign_a, 1 + odd), (wb, -sign_a, 2 - odd)):
        cx = sign * cxd
        multiplier = jnp.where(d == row, courant * cxd, common)
        ypow = [1.0, cy, cy * cy, cy * cy * cy]
        zpow = [1.0, cz, cz * cz, cz * cz * cz]
        xpow = [1.0, cx, cx * cx, cx * cx * cx]
        for k, terms in enumerate(MOMENTS):
            phi = 0.0
            for ax, ay, az in terms:
                phi = phi + xpow[ax] * (ypow[ay] * zpow[az])
            w[8 * k : 8 * k + 8, :] = multiplier * phi
        w[8 * NK : ROWS, :] = jnp.zeros((8, HALF), f32)
    edge = jnp.where(jnp.logical_or(x == 0, x == 7), 1.0, 0.0)
    sub = lax.broadcasted_iota(jnp.int32, (8, CELLS), 0)
    temp = jnp.broadcast_to(temp_ref[pl.ds(face, 1), :], (8, CELLS))
    kind = jnp.broadcast_to(type_ref[pl.ds(face, 1), :], (8, CELLS))
    for k, value in enumerate(wall_moments(temp, tables[face])):
        wall[8 * k : 8 * k + 8, :] = value
    two_pi = 2.0 * np.pi * temp
    rows = jnp.where(sub == 0, jnp.where(kind == 1, edge, 0.0), 0.0)
    rows = jnp.where(sub == 1, jnp.where(kind == 2, edge, 0.0), rows)
    rows = jnp.where(sub == 2, -0.5 / temp, rows)
    rows = jnp.where(sub == 3, box_volume / (two_pi * jnp.sqrt(two_pi)), rows)
    cols[...] = to_columns(rows)
    cy16, cz16 = lane_speeds(p, 16)
    speed_sq = cy16 * cy16 + cz16 * cz16 + cxd * cxd

    def step(i, carry):
        at = pl.ds(pl.multiple_of(i * 16, 16), 16)
        c = cols[at, :]
        wall_bulk[at, :] = c[:, 3:4] * jnp.exp(speed_sq * c[:, 2:3])
        return carry

    lax.fori_loop(0, 16, step, 0, unroll=4)
    flux = dot_t(jnp.full((8, HALF), 1.0, f32), fb[...]) * cxd
    pre[8 * NK : ROWS, :] = flux * edge
    copy.wait()
    in_rows = dot_t(wa[...], infl[...])
    for k in range(NK):
        pick = jnp.where(odd == 1, in_rows[8 * k + 2 : 8 * k + 3], in_rows[8 * k + 1 : 8 * k + 2])
        pre[8 * k : 8 * k + 8, :] = jnp.where(sub == 7, jnp.broadcast_to(pick, (8, CELLS)), 0.0) * edge


def upwind_y(p, i):
    return pl.ds(pl.multiple_of(((i + jnp.where(p % 2 == 1, 15, 1)) % 16) * 16, 16), 16)


def transport_weights(cxd, cy, cz):
    abs_y, abs_z = courant * jnp.abs(cy), courant * jnp.abs(cz)
    return 1.0 - courant * cxd - abs_y - abs_z, courant * cxd, abs_y, abs_z, cz > 0.0


def transport_block(value, neighbour_y, plane, weights):
    centre, abs_x, abs_y, abs_z, forward = weights
    neighbour_z = jnp.where(forward, pltpu.roll(value, 1, 0), pltpu.roll(value, 15, 0))
    return value * centre + abs_x * plane + abs_y * neighbour_y + abs_z * neighbour_z


def read_kernel(fa, fb, ha, hb, infl, cols, wa, wb, pre, ra, rb, keep, send):
    x, p = here()
    edge = jnp.where(jnp.logical_or(x == 0, x == 7), 1.0, 0.0)
    weights = transport_weights(speed_x(p), *lane_speeds(p, 16))

    def step(i, carry):
        at = pl.ds(pl.multiple_of(i * 16, 16), 16)
        up = upwind_y(p, i)
        c = cols[at, :]
        value = fa[at, :]
        plane = hb[at, :] * (1.0 - edge) + infl[at, :] * c[:, 0:1] + c[:, 1:2] * value
        ra[at, :] = transport_block(value, fa[up, :], plane, weights)
        rb[at, :] = transport_block(fb[at, :], fb[up, :], ha[at, :], weights)
        return carry

    lax.fori_loop(0, 16, step, 0, unroll=4)
    rows = pre[...] + dot_t(wa[...], ra[...]) + dot_t(wb[...], rb[...])
    north = p % 2 == 1
    top, bottom = rows[:HROWS], rows[HROWS:]
    keep[...] = jnp.where(north, bottom, top)
    send[...] = jnp.where(north, top, bottom)


def cell_kernel(mine, other, wall, type_ref, table, send_a, send_b, own, state):
    x, p = here()
    upper = x == 7
    odd = x % 2 == 1
    face = jnp.where(x >= 4, 1, 0)
    edge = jnp.where(jnp.logical_or(x == 0, upper), 1.0, 0.0)
    north = p % 2 == 1
    a, b = mine[...], other[...]
    rows = jnp.concatenate([jnp.where(north, b, a), jnp.where(north, a, b)], 0)
    m = [rows[8 * k : 8 * k + 8] for k in range(NK)]
    plain = [wall[8 * k : 8 * k + 8, :] for k in range(NK)]
    kind = jnp.broadcast_to(type_ref[pl.ds(face, 1), :], (8, CELLS))
    is_wall = jnp.where(kind == 0, edge, 0.0)
    is_in = jnp.where(kind == 1, edge, 0.0)
    is_out = jnp.where(kind == 2, edge, 0.0)

    def first(v):
        return jnp.where(odd, v[2:3], v[1:2])

    def second(v):
        return jnp.where(odd, v[1:2], v[2:3])

    entering = spread(first(plain[0])) * (1.0 / courant)
    amp = is_wall * spread(rows[8 * NK : 8 * NK + 1]) / entering
    inflow = [v[7:8] for v in m]
    m = [v + amp * wall[8 * (NK + k) : 8 * (NK + k) + 8, :] for k, v in enumerate(m)]
    params, rate = relax_params([spread(v[:1]) for v in m], table[...])
    s = equilibrium_moments(params, table[...])
    inv = 1.0 / (1.0 + rate)
    m = [(v + rate * w) * inv for v, w in zip(m, s)]
    amp2 = is_wall * spread(second(m[0])) * (1.0 / courant) / entering
    sub = lax.broadcasted_iota(jnp.int32, (8, CELLS), 0)
    lane = lax.broadcasted_iota(jnp.int32, (8, CELLS), 1)
    low, high = lane % 16 == 0, lane % 16 == 15
    for k in range(NK):
        v = m[k]
        z_up = jnp.where(low, pltpu.roll(v, CELLS - 15, 1), pltpu.roll(v, 1, 1))
        z_down = jnp.where(high, pltpu.roll(v, 15, 1), pltpu.roll(v, CELLS - 1, 1))
        total = jnp.where(sub == 0, v, jnp.where(sub == 7, 0.0, -v))
        total = total + jnp.where(sub == 3, pltpu.roll(v, 16, 1), 0.0)
        total = total + jnp.where(sub == 4, pltpu.roll(v, CELLS - 16, 1), 0.0)
        total = total + jnp.where(sub == 5, z_up, 0.0) + jnp.where(sub == 6, z_down, 0.0)
        va = first(v)
        ghost = amp2[:1] * first(plain[k]) + is_in[:1] * inflow[k] + is_out[:1] * va
        own[k : k + 1, :] = jnp.sum(total, 0, keepdims=True) + ghost
        send_a[k : k + 1, :] = va
        send_b[k : k + 1, :] = second(v)
    own[NK:16, :] = jnp.zeros((3, CELLS), f32)
    extra = list(params) + [rate, amp]
    for k, v in enumerate(extra):
        send_a[NK + k : NK + k + 1, :] = v[:1]
        send_b[NK + k : NK + k + 1, :] = v[:1]
        state[k : k + 1, :] = v[:1]
    send_a[23:24, :] = jnp.zeros((1, CELLS), f32)
    send_b[23:24, :] = jnp.zeros((1, CELLS), f32)
    state[10:11, :] = amp2[:1]
    state[11:16, :] = jnp.zeros((5, CELLS), f32)


NCOL = 16


def bulk_rows(params, rate, cx_a, cx_b, extra=()):
    n, ux, uy, uz, temp, qx, qy, qz = params
    inv = 1.0 / temp
    two_pi = 2.0 * np.pi * temp
    share = 1.0 / (1.0 + rate)
    scale = inv * inv / (15.0 * n)
    pref = rate * share * n * box_volume / (two_pi * jnp.sqrt(two_pi))
    rows = [uy, uz, -0.5 * inv, inv, qy * scale, qz * scale, share]
    for cx in (cx_a, cx_b):
        w = cx - ux
        square = w * w
        rows += [pref * jnp.exp(-0.5 * inv * square), qx * scale * w, square * inv]
    rows += list(extra)
    return rows + [jnp.zeros((1, CELLS), f32)] * (NCOL - len(rows))


def columns(c, base):
    return [c[:, base + j : base + j + 1] for j in range(NCOL)]


def shared_part(k, cy, cz):
    wy = cy - k[0]
    wz = cz - k[1]
    square = wy * wy + wz * wz
    return jnp.exp(square * k[2]), square * k[3] - 5.0, wy * k[4] + wz * k[5]


def relaxed(value, k, part, half):
    decay, square, heat = part
    pref, heat_x, square_x = k[7 + 3 * half : 10 + 3 * half]
    return value * k[6] + (decay * pref) * (1.0 + (heat + heat_x) * (square + square_x))


def own_kernel(ra, rb, state, wall_bulk, ca, cb, work):
    x, p = here()
    cxd = speed_x(p)
    sign_a = jnp.where(x % 2 == 0, 1.0, -1.0)
    cy, cz = lane_speeds(p, 16)
    st = state[...]
    rows = bulk_rows(
        [st[k : k + 1] for k in range(8)], st[8:9], sign_a * cxd, -sign_a * cxd, [st[9:10] * (courant * cxd)]
    )
    work[...] = to_columns(jnp.concatenate(rows, 0))

    def step(i, carry):
        at = pl.ds(pl.multiple_of(i * 16, 16), 16)
        k = columns(work[at, :], 0)
        part = shared_part(k, cy, cz)
        ca[at, :] = relaxed(ra[at, :] + k[13] * wall_bulk[at, :], k, part, 0)
        cb[at, :] = relaxed(rb[at, :], k, part, 1)
        return carry

    lax.fori_loop(0, 16, step, 0, unroll=4)


def final_kernel(
    ca, cb, ha, hb, from_a, from_b, own, state, wall_bulk, infl, cols, table, out, fields, pa, pb, oa, ob, work, sems
):
    x, p = here()
    odd = x % 2
    cxd = speed_x(p)
    sign_a = jnp.where(odd == 0, 1.0, -1.0)
    cx_a, cx_b = sign_a * cxd, -sign_a * cxd
    cy, cz = lane_speeds(p, 16)
    weights = transport_weights(cxd, cy, cz)
    edge = jnp.where(jnp.logical_or(x == 0, x == 7), 1.0, 0.0)
    ta, tb, st = from_a[...], from_b[...], state[...]
    m = [spread(own[k : k + 1, :] + ta[k : k + 1] + tb[k : k + 1]) for k in range(NK)]
    params, rate = relax_params(m, table[...])
    wall_scale = courant * cxd
    tb = jnp.where(edge > 0.0, st[:10], tb[NK : NK + 10])
    ta = ta[NK : NK + 10]

    def coefficients(source, extra=()):
        return bulk_rows([source[k : k + 1] for k in range(8)], source[8:9], cx_a, cx_b, extra)

    rows = coefficients(ta, [ta[9:10] * wall_scale])
    rows += coefficients(tb, [jnp.zeros((1, CELLS), f32), st[10:11]])
    rows += bulk_rows([v[:1] for v in params], rate[:1], cx_a, cx_b)
    work[...] = to_columns(jnp.concatenate(rows, 0))

    def first(i, carry):
        at = pl.ds(pl.multiple_of(i * 16, 16), 16)
        c = work[at, :]
        k = cols[at, :]
        w = wall_bulk[at, :]
        ka, kb = columns(c, 0), columns(c, NCOL)
        halo = relaxed(hb[at, :], kb, shared_part(kb, cy, cz), 0)
        pa[at, :] = (1.0 - edge) * halo + infl[at, :] * k[:, 0:1] + kb[14] * w + k[:, 1:2] * ca[at, :]
        pb[at, :] = relaxed(ha[at, :] + ka[13] * w, ka, shared_part(ka, cy, cz), 1)
        return carry

    lax.fori_loop(0, 16, first, 0, unroll=4)
    copies = []
    for chunk in range(4):

        def second(i, carry):
            at = pl.ds(pl.multiple_of(i * 16, 16), 16)
            up = upwind_y(p, i)
            k = columns(work[at, :], 2 * NCOL)
            part = shared_part(k, cy, cz)
            read = transport_block(ca[at, :], ca[up, :], pa[at, :], weights)
            oa[at, :] = relaxed(read, k, part, 0)
            read = transport_block(cb[at, :], cb[up, :], pb[at, :], weights)
            ob[at, :] = relaxed(read, k, part, 1)
            return carry

        lax.fori_loop(4 * chunk, 4 * chunk + 4, second, 0, unroll=4)
        at = pl.ds(64 * chunk, 64)
        for half, source, start in ((0, oa, 1 - odd), (1, ob, odd)):
            copy = pltpu.make_async_copy(
                source.at[at, :], out.at[at, pl.ds(half_start(start), HALF)], sems.at[2 * chunk + half]
            )
            copy.start()
            copies.append(copy)
    table8 = jnp.concatenate([v[:1] for v in params], 0)
    for y in range(16):
        fields[:, y, :] = table8[:, 16 * y : 16 * y + 16]
    for copy in copies:
        copy.wait()


VMEM = pl.BlockSpec(memory_space=pltpu.VMEM)
ANY = pl.BlockSpec(memory_space=pl.ANY)
PLANE = (CELLS, HALF)


def call(kernel, outs, args, scratch=(), sems=0, loose_in=(), loose_out=(), cost=1_000_000, grant=16):
    scratches = [pltpu.VMEM(s, f32) for s in scratch]
    if sems:
        scratches.append(pltpu.SemaphoreType.DMA((sems,)))
    return pl.pallas_call(
        kernel,
        out_shape=[jax.ShapeDtypeStruct(s, f32) for s in outs],
        in_specs=[ANY if k in loose_in else VMEM for k in range(len(args))],
        out_specs=[ANY if k in loose_out else VMEM for k in range(len(outs))],
        scratch_shapes=scratches,
        cost_estimate=pl.CostEstimate(flops=cost, bytes_accessed=1 << 20, transcendentals=0),
        compiler_params=pltpu.CompilerParams(vmem_limit_bytes=grant << 20),
    )(*args)


PAIRS_A = [(i, i ^ 1) for i in range(8)]
PAIRS_B = [pair for i in (1, 3, 5) for pair in ((i, i + 1), (i + 1, i))]
SWAP = [(0, 1), (1, 0)]


def both_ways(pairs):
    return [pair for i, j in pairs for pair in ((i, j), (j, i))]


Z_ROUNDS = [
    ("zround1", both_ways([(0, 1), (2, 3), (4, 5), (6, 7)])),
    ("zround2", both_ways([(0, 2), (1, 3), (4, 6), (5, 7)])),
    ("zround3", both_ways([(0, 6), (1, 7), (2, 4), (3, 5)])),
]


def swap_planes(a, b):
    b = lax.ppermute(b, "space", PAIRS_B)
    a = lax.ppermute(a, "space", PAIRS_A)
    return a, b


def body(distribution, inflow, wall_temp, face_type):
    f = distribution.reshape(CELLS, 2 * HALF)
    fa, fb = call(split_kernel, [PLANE, PLANE], [f], sems=2, loose_in=(0,))
    ha, hb = swap_planes(fa, fb)
    temp = wall_temp.reshape(2, CELLS)
    kind = face_type.reshape(2, CELLS)
    table = jnp.asarray(TABLE)
    infl, wa, wb, pre, wall, wall_bulk, cols = call(
        setup_kernel,
        [PLANE, (ROWS, HALF), (ROWS, HALF), (ROWS, CELLS), (2 * NK * 8, CELLS), PLANE, (CELLS, 128)],
        [inflow.reshape(2, CELLS, 2 * HALF), fb, temp, kind, jnp.asarray(WALL_TABLES)],
        sems=1,
        loose_in=(0,),
    )
    ra, rb, keep, send = call(
        read_kernel,
        [PLANE, PLANE, (HROWS, CELLS), (HROWS, CELLS)],
        [fa, fb, ha, hb, infl, cols, wa, wb, pre],
    )
    part = keep + lax.ppermute(send, "core", SWAP)
    part = part + lax.ppermute(part, "ylo", SWAP)
    ga = lax.optimization_barrier((ra, part))[0]
    gb = rb
    for name, pairs in Z_ROUNDS:
        if name == "zround2":
            gb = lax.optimization_barrier((rb, part))[0]
        part = part + lax.ppermute(part, "z", pairs)
    ga, gb = swap_planes(ga, gb)
    other = lax.ppermute(part, "core", SWAP)
    send_a, send_b, own, state = call(
        cell_kernel,
        [(24, CELLS), (24, CELLS), (16, CELLS), (16, CELLS)],
        [part, other, wall, kind, table],
    )
    from_a, from_b = swap_planes(send_a, send_b)
    ca, cb = call(own_kernel, [PLANE, PLANE], [ra, rb, state, wall_bulk], scratch=[(CELLS, 128)], cost=40_000_000)
    out, fields = call(
        final_kernel,
        [(CELLS, 2 * HALF), (8, 16, 16)],
        [ca, cb, ga, gb, from_a, from_b, own, state, wall_bulk, infl, cols, table],
        scratch=[PLANE] * 4 + [(CELLS, 128)],
        sems=8,
        loose_out=(0,),
    )
    return out.reshape(1, 16, 16, 2 * HALF), fields[:, None]


def solution(mesh):
    split = Mesh(mesh.devices.reshape(8, 8, 2, 2), ("space", "z", "ylo", "core"))
    vel = ("z", "ylo", "core")
    in_specs = (P("space", None, None, vel), P(None, None, None, vel), P(), P())
    out_specs = (P("space", None, None, vel), P(None, "space", None, None))

    return jax.shard_map(body, mesh=split, in_specs=in_specs, out_specs=out_specs, check_vma=False)
```

```python
import jax
import jax.numpy as jnp
import numpy as np
from jax import lax
from jax.experimental import pallas as pl
from jax.experimental.pallas import tpu as pltpu
from jax.sharding import Mesh, PartitionSpec as P


NV = 32768
CELLS = 256
HALF = 512
NK = 13
ROWS = 96
HROWS = ROWS // 2
courant = 0.08
rate_field = 0.8
box_volume = 512.0
HIGHEST = lax.Precision.HIGHEST
f32 = jnp.float32

MOMENTS = [
    [(0, 0, 0)],
    [(1, 0, 0)],
    [(0, 1, 0)],
    [(0, 0, 1)],
    [(2, 0, 0)],
    [(0, 2, 0)],
    [(0, 0, 2)],
    [(1, 1, 0)],
    [(1, 0, 1)],
    [(0, 1, 1)],
    [(3, 0, 0), (1, 2, 0), (1, 0, 2)],
    [(2, 1, 0), (0, 3, 0), (0, 1, 2)],
    [(2, 0, 1), (0, 2, 1), (0, 0, 3)],
]


def axis_table(top):
    grid = (np.arange(32) + 0.5) * 0.25 - 4.0
    plus, minus = courant * np.maximum(grid, 0.0), courant * np.maximum(-grid, 0.0)
    table = np.zeros((24 * top, 96))
    for axis in range(3):
        for power in range(top):
            for d in range(7):
                row = grid**power
                if d == 1 + 2 * axis:
                    row = row * plus
                if d == 2 + 2 * axis:
                    row = row * minus
                table[8 * top * axis + 8 * power + d, 32 * axis : 32 * axis + 32] = row
    return table.astype(np.float32), plus, minus


def wall_tables():
    table, plus, minus = axis_table(4)
    walls = []
    for weight in (plus, minus):
        wall = table.copy()
        wall[:32, :32] *= weight
        walls.append(np.concatenate([table, wall]))
    return np.stack(walls).astype(np.float32)


TOP = 7
TABLE = axis_table(TOP)[0]
WALL_TABLES = wall_tables()


def dot(a, b):
    return lax.dot_general(a, b, (((1,), (0,)), ((), ())), precision=HIGHEST, preferred_element_type=f32)


def dot_t(a, b):
    return lax.dot_general(a, b, (((1,), (1,)), ((), ())), precision=HIGHEST, preferred_element_type=f32)


def tile4(a):
    return jnp.concatenate([a] * 4, 0)


def speed_grid():
    return (lax.broadcasted_iota(jnp.int32, (32, CELLS), 0).astype(f32) + 0.5) * 0.25 - 4.0


def lane_speeds(p, rows):
    lane = lax.broadcasted_iota(jnp.int32, (rows, HALF), 1)
    cy = ((lane // 32 + (p % 2) * 16).astype(f32) + 0.5) * 0.25 - 4.0
    cz = ((lane % 32).astype(f32) + 0.5) * 0.25 - 4.0
    return cy, cz


def speed_x(p):
    return ((p // 2).astype(f32) + 0.5) * 0.25


def to_columns(rows):
    pad = 128 - rows.shape[0]
    return jnp.transpose(jnp.concatenate([rows, jnp.zeros((pad, CELLS), f32)], 0))


def equilibrium_moments(params, table):
    n, ux, uy, uz, temp, qx, qy, qz = params
    inv = 1.0 / temp
    two_pi = 2.0 * np.pi * temp
    pref = n * box_volume / (two_pi * jnp.sqrt(two_pi))
    scale = inv * inv / (15.0 * n)
    grid = speed_grid()
    decay = tile4(-0.5 * inv)
    decays = []
    for u in (ux, uy, uz):
        w = grid - tile4(u)
        decays.append(jnp.exp(w * w * decay))
    sums = dot(table, jnp.concatenate(decays, 0))
    factors = []
    for axis, (u, q) in enumerate(((ux, qx), (uy, qy), (uz, qz))):
        kq = q * scale
        base = 8 * TOP * axis
        levels = [[sums[base + 8 * a : base + 8 * a + 8] for a in range(TOP)]]
        for _ in range(3):
            last = levels[-1]
            levels.append([last[a + 1] - u * last[a] for a in range(len(last) - 1)])
        powers = []
        for power in range(4):
            t0, t1, t2, t3 = [level[power] for level in levels]
            powers.append((t0, kq * t1, t2 * inv, kq * (t3 * inv - 5.0 * t1)))
        factors.append(powers)
    xs, ys, zs = factors
    pairs = {}

    def pair(ay, az):
        if (ay, az) not in pairs:
            y0, y1, y2, y3 = ys[ay]
            z0, z1, z2, z3 = zs[az]
            a = y0 * z0
            b = a + y3 * z0 + y0 * z3 + y1 * z2 + y2 * z1
            pairs[(ay, az)] = (a, b, y2 * z0 + y0 * z2, y1 * z0 + y0 * z1)
        return pairs[(ay, az)]

    out = []
    for terms in MOMENTS:
        total = 0.0
        for ax, ay, az in terms:
            x0, x1, x2, x3 = xs[ax]
            a, b, c, d = pair(ay, az)
            total = total + (x0 * b + x3 * a + x1 * c + x2 * d)
        out.append(pref * total)
    return out


def wall_moments(temp, tables):
    grid = speed_grid()
    g = jnp.exp(grid * grid * tile4(-0.5 / temp))
    sums = dot(tables, jnp.concatenate([g] * 3, 0))
    two_pi = 2.0 * np.pi * temp
    pref = box_volume / (two_pi * jnp.sqrt(two_pi))
    out = []
    for base in (0, 96):
        for terms in MOMENTS:
            total = 0.0
            for powers in terms:
                part = pref
                for axis in range(3):
                    row = base + 32 * axis + 8 * powers[axis]
                    part = part * sums[row : row + 8]
                total = total + part
            out.append(total)
    return out


def macro(m):
    m = [a * (1.0 / NV) for a in m]
    n = m[0]
    rn = 1.0 / n
    ux, uy, uz = m[1] * rn, m[2] * rn, m[3] * rn
    square = ux * ux + uy * uy + uz * uz
    energy = m[4] + m[5] + m[6]
    temp = (energy - n * square) * rn * (1.0 / 3.0)
    lift = 2.0 * n * square - energy
    qx = 0.5 * (m[10] + ux * lift) - (ux * m[4] + uy * m[7] + uz * m[8])
    qy = 0.5 * (m[11] + uy * lift) - (ux * m[7] + uy * m[5] + uz * m[9])
    qz = 0.5 * (m[12] + uz * lift) - (ux * m[8] + uy * m[9] + uz * m[6])
    rate = rate_field * n * jnp.exp(0.19 * jnp.log(temp))
    return (n, ux, uy, uz, temp, qx, qy, qz), rate


def spread(row):
    return jnp.broadcast_to(row, (8, CELLS))


def relax_params(m, table):
    params, rate = macro(m)
    for _ in range(2):
        s = [spread(a[:1]) for a in equilibrium_moments(params, table)]
        inv = 1.0 / (1.0 + rate)
        params, rate = macro([(a + rate * b) * inv for a, b in zip(m, s)])
    return params, rate


def here():
    x = lax.axis_index("space")
    p = lax.axis_index("z") * 4 + lax.axis_index("ylo") * 2 + lax.axis_index("core")
    return x, p


def half_start(index):
    return pl.multiple_of(index * HALF, HALF)


def split_kernel(f, fa, fb, sems):
    x, _ = here()
    odd = x % 2
    first = pltpu.make_async_copy(f.at[:, pl.ds(half_start(1 - odd), HALF)], fa, sems.at[0])
    second = pltpu.make_async_copy(f.at[:, pl.ds(half_start(odd), HALF)], fb, sems.at[1])
    first.start()
    second.start()
    first.wait()
    second.wait()


def setup_kernel(inflow, fb, temp_ref, type_ref, tables, infl, wa, wb, pre, wall, wall_bulk, cols, sems):
    x, p = here()
    odd = x % 2
    face = jnp.where(x >= 4, 1, 0)
    copy = pltpu.make_async_copy(inflow.at[face, :, pl.ds(half_start(1 - odd), HALF)], infl, sems.at[0])
    copy.start()
    cxd = speed_x(p)
    cy, cz = lane_speeds(p, 8)
    d = lax.broadcasted_iota(jnp.int32, (8, HALF), 0)
    yp, ym = courant * jnp.maximum(cy, 0.0), courant * jnp.maximum(-cy, 0.0)
    zp, zm = courant * jnp.maximum(cz, 0.0), courant * jnp.maximum(-cz, 0.0)
    sign_a = jnp.where(odd == 0, 1.0, -1.0)
    for w, sign in ((wa, sign_a), (wb, -sign_a)):
        cx = sign * cxd
        xp, xm = courant * jnp.maximum(cx, 0.0), courant * jnp.maximum(-cx, 0.0)
        plus = jnp.where(d == 0, 1.0, jnp.where(d == 1, xp, jnp.where(d == 3, yp, jnp.where(d == 5, zp, 0.0))))
        full = jnp.where(d == 2, xm, jnp.where(d == 4, ym, jnp.where(d == 6, zm, plus)))
        ypow = [1.0, cy, cy * cy, cy * cy * cy]
        zpow = [1.0, cz, cz * cz, cz * cz * cz]
        xpow = [1.0, cx, cx * cx, cx * cx * cx]
        phis = []
        for terms in MOMENTS:
            phi = 0.0
            for ax, ay, az in terms:
                phi = phi + xpow[ax] * (ypow[ay] * zpow[az])
            phis.append(phi)
        gaps = jnp.where(d == 2, xp, jnp.where(d == 4, yp, jnp.where(d == 6, zp, 0.0)))
        w[0:8, :] = plus * phis[0] + gaps * phis[3]
        w[8:16, :] = plus * phis[1] + jnp.where(d == 2, phis[3], 0.0)
        w[16:24, :] = plus * phis[2]
        for k in range(4, NK):
            w[8 * k - 8 : 8 * k, :] = full * phis[k]
    edge = jnp.where(jnp.logical_or(x == 0, x == 7), 1.0, 0.0)
    sub = lax.broadcasted_iota(jnp.int32, (8, CELLS), 0)
    temp = jnp.broadcast_to(temp_ref[pl.ds(face, 1), :], (8, CELLS))
    kind = jnp.broadcast_to(type_ref[pl.ds(face, 1), :], (8, CELLS))
    for k, value in enumerate(wall_moments(temp, tables[face])):
        wall[8 * k : 8 * k + 8, :] = value
    two_pi = 2.0 * np.pi * temp
    rows = jnp.where(sub == 0, jnp.where(kind == 1, edge, 0.0), 0.0)
    rows = jnp.where(sub == 1, jnp.where(kind == 2, edge, 0.0), rows)
    rows = jnp.where(sub == 2, -0.5 / temp, rows)
    rows = jnp.where(sub == 3, box_volume / (two_pi * jnp.sqrt(two_pi)), rows)
    cols[...] = to_columns(rows)
    cy16, cz16 = lane_speeds(p, 16)
    speed_sq = cy16 * cy16 + cz16 * cz16 + cxd * cxd

    def step(i, carry):
        at = pl.ds(pl.multiple_of(i * 16, 16), 16)
        c = cols[at, :]
        wall_bulk[at, :] = c[:, 3:4] * jnp.exp(speed_sq * c[:, 2:3])
        return carry

    lax.fori_loop(0, 16, step, 0, unroll=4)
    flux = dot_t(jnp.full((8, HALF), 1.0, f32), fb[...]) * (cxd * edge)
    copy.wait()
    in_rows = dot_t(wa[...], infl[...]) * (courant * cxd * edge)
    for group in range(ROWS // 8):
        value = jnp.where(sub == 7, spread(in_rows[8 * group : 8 * group + 1]), 0.0)
        if group == 1:
            value = jnp.where(sub == 6, spread(in_rows[10:11]), jnp.where(sub == 4, flux, value))
        pre[8 * group : 8 * group + 8, :] = value


def upwind_y(p, i):
    return pl.ds(pl.multiple_of(((i + jnp.where(p % 2 == 1, 15, 1)) % 16) * 16, 16), 16)


def transport_weights(cxd, cy, cz):
    abs_y, abs_z = courant * jnp.abs(cy), courant * jnp.abs(cz)
    return 1.0 - courant * cxd - abs_y - abs_z, courant * cxd, abs_y, abs_z, cz > 0.0


def transport_block(value, neighbour_y, plane, weights):
    centre, abs_x, abs_y, abs_z, forward = weights
    neighbour_z = jnp.where(forward, pltpu.roll(value, 1, 0), pltpu.roll(value, 15, 0))
    return value * centre + abs_x * plane + abs_y * neighbour_y + abs_z * neighbour_z


def read_b_kernel(fb, ha, wb, pre, rb, rows):
    _, p = here()
    weights = transport_weights(speed_x(p), *lane_speeds(p, 16))

    def step(i, carry):
        at = pl.ds(pl.multiple_of(i * 16, 16), 16)
        rb[at, :] = transport_block(fb[at, :], fb[upwind_y(p, i), :], ha[at, :], weights)
        return carry

    lax.fori_loop(0, 16, step, 0, unroll=4)
    rows[...] = pre[...] + dot_t(wb[...], rb[...])


def read_a_kernel(fa, hb, infl, cols, wa, rows_b, ra, keep, send):
    x, p = here()
    inner = jnp.where(jnp.logical_or(x == 0, x == 7), 0.0, 1.0)
    weights = transport_weights(speed_x(p), *lane_speeds(p, 16))

    def step(i, carry):
        at = pl.ds(pl.multiple_of(i * 16, 16), 16)
        c = cols[at, :]
        value = fa[at, :]
        plane = hb[at, :] * inner + infl[at, :] * c[:, 0:1] + c[:, 1:2] * value
        ra[at, :] = transport_block(value, fa[upwind_y(p, i), :], plane, weights)
        return carry

    lax.fori_loop(0, 16, step, 0, unroll=4)
    rows = rows_b[...] + dot_t(wa[...], ra[...])
    north = p % 2 == 1
    top, bottom = rows[:HROWS], rows[HROWS:]
    keep[...] = jnp.where(north, bottom, top)
    send[...] = jnp.where(north, top, bottom)


def unpack_rows(groups, sub):
    first, second = groups[0], groups[1]
    plain = [groups[0][:1], groups[1][:1], groups[2][:1], groups[1][2:3]] + [g[:1] for g in groups[3:]]
    odd = jnp.logical_or(sub == 1, jnp.logical_or(sub == 3, sub == 5))
    even = jnp.logical_or(sub == 2, jnp.logical_or(sub == 4, sub == 6))
    products = [(1, 2, 3), (4, 7, 8), (7, 5, 9), (8, 9, 6)]

    def less(plus, k):
        ix, iy, iz = products[k]
        change = jnp.where(sub == 2, spread(plain[ix]), jnp.where(sub == 4, spread(plain[iy]), spread(plain[iz])))
        return plus - courant * change

    out = []
    for k in range(3):
        out.append(jnp.where(even, less(pltpu.roll(groups[k], 1, 0), k), groups[k]))
    rest = jnp.where(sub == 0, spread(second[2:3]), spread(second[6:7]))
    out.append(jnp.where(odd, pltpu.roll(first, 7, 0), jnp.where(even, less(first, 3), rest)))
    return out + list(groups[3:]), second[4:5]


def cell_kernel(mine, other, wall, type_ref, table, send_a, send_b, own, state):
    x, p = here()
    upper = x == 7
    odd = x % 2 == 1
    face = jnp.where(x >= 4, 1, 0)
    edge = jnp.where(jnp.logical_or(x == 0, upper), 1.0, 0.0)
    north = p % 2 == 1
    a, b = mine[...], other[...]
    rows = jnp.concatenate([jnp.where(north, b, a), jnp.where(north, a, b)], 0)
    sub = lax.broadcasted_iota(jnp.int32, (8, CELLS), 0)
    m, leaving = unpack_rows([rows[8 * k : 8 * k + 8] for k in range(ROWS // 8)], sub)
    plain = [wall[8 * k : 8 * k + 8, :] for k in range(NK)]
    kind = jnp.broadcast_to(type_ref[pl.ds(face, 1), :], (8, CELLS))
    is_wall = jnp.where(kind == 0, edge, 0.0)
    is_in = jnp.where(kind == 1, edge, 0.0)
    is_out = jnp.where(kind == 2, edge, 0.0)

    def first(v):
        return jnp.where(odd, v[2:3], v[1:2])

    def second(v):
        return jnp.where(odd, v[1:2], v[2:3])

    entering = spread(first(plain[0])) * (1.0 / courant)
    amp = is_wall * spread(leaving) / entering
    inflow = [v[7:8] for v in m]
    m = [v + amp * wall[8 * (NK + k) : 8 * (NK + k) + 8, :] for k, v in enumerate(m)]
    params, rate = relax_params([spread(v[:1]) for v in m], table[...])
    s = equilibrium_moments(params, table[...])
    inv = 1.0 / (1.0 + rate)
    m = [(v + rate * w) * inv for v, w in zip(m, s)]
    amp2 = is_wall * spread(second(m[0])) * (1.0 / courant) / entering
    lane = lax.broadcasted_iota(jnp.int32, (8, CELLS), 1)
    low, high = lane % 16 == 0, lane % 16 == 15
    for k in range(NK):
        v = m[k]
        z_up = jnp.where(low, pltpu.roll(v, CELLS - 15, 1), pltpu.roll(v, 1, 1))
        z_down = jnp.where(high, pltpu.roll(v, 15, 1), pltpu.roll(v, CELLS - 1, 1))
        total = jnp.where(sub == 0, v, jnp.where(sub == 7, 0.0, -v))
        total = total + jnp.where(sub == 3, pltpu.roll(v, 16, 1), 0.0)
        total = total + jnp.where(sub == 4, pltpu.roll(v, CELLS - 16, 1), 0.0)
        total = total + jnp.where(sub == 5, z_up, 0.0) + jnp.where(sub == 6, z_down, 0.0)
        va = first(v)
        ghost = amp2[:1] * first(plain[k]) + is_in[:1] * inflow[k] + is_out[:1] * va
        own[k : k + 1, :] = jnp.sum(total, 0, keepdims=True) + ghost
        send_a[k : k + 1, :] = va
        send_b[k : k + 1, :] = second(v)
    own[NK:16, :] = jnp.zeros((3, CELLS), f32)
    extra = list(params) + [rate, amp]
    for k, v in enumerate(extra):
        send_a[NK + k : NK + k + 1, :] = v[:1]
        send_b[NK + k : NK + k + 1, :] = v[:1]
        state[k : k + 1, :] = v[:1]
    send_a[23:24, :] = jnp.zeros((1, CELLS), f32)
    send_b[23:24, :] = jnp.zeros((1, CELLS), f32)
    state[10:11, :] = amp2[:1]
    state[11:16, :] = jnp.zeros((5, CELLS), f32)


NCOL = 16


def bulk_rows(params, rate, cx_a, cx_b, extra=()):
    n, ux, uy, uz, temp, qx, qy, qz = params
    inv = 1.0 / temp
    two_pi = 2.0 * np.pi * temp
    share = 1.0 / (1.0 + rate)
    scale = inv * inv / (15.0 * n)
    pref = rate * share * n * box_volume / (two_pi * jnp.sqrt(two_pi))
    rows = [uy, uz, -0.5 * inv, inv, qy * scale, qz * scale, share]
    for cx in (cx_a, cx_b):
        w = cx - ux
        square = w * w
        rows += [pref * jnp.exp(-0.5 * inv * square), qx * scale * w, square * inv]
    rows += list(extra)
    return rows + [jnp.zeros((1, CELLS), f32)] * (NCOL - len(rows))


def columns(c, base):
    return [c[:, base + j : base + j + 1] for j in range(NCOL)]


def shared_part(k, cy, cz):
    wy = cy - k[0]
    wz = cz - k[1]
    square = wy * wy + wz * wz
    return jnp.exp(square * k[2]), square * k[3] - 5.0, wy * k[4] + wz * k[5]


def relaxed(value, k, part, half):
    decay, square, heat = part
    pref, heat_x, square_x = k[7 + 3 * half : 10 + 3 * half]
    return value * k[6] + (decay * pref) * (1.0 + (heat + heat_x) * (square + square_x))


def own_kernel(ra, rb, state, wall_bulk, infl, cols, ca, cb, ghost, work):
    x, p = here()
    cxd = speed_x(p)
    sign_a = jnp.where(x % 2 == 0, 1.0, -1.0)
    cy, cz = lane_speeds(p, 16)
    st = state[...]
    rows = bulk_rows(
        [st[k : k + 1] for k in range(8)], st[8:9], sign_a * cxd, -sign_a * cxd, [st[9:10] * (courant * cxd), st[10:11]]
    )
    work[...] = to_columns(jnp.concatenate(rows, 0))

    def step(i, carry):
        at = pl.ds(pl.multiple_of(i * 16, 16), 16)
        k = columns(work[at, :], 0)
        part = shared_part(k, cy, cz)
        face = cols[at, :]
        w = wall_bulk[at, :]
        value = relaxed(ra[at, :] + k[13] * w, k, part, 0)
        ca[at, :] = value
        cb[at, :] = relaxed(rb[at, :], k, part, 1)
        ghost[at, :] = infl[at, :] * face[:, 0:1] + k[14] * w + face[:, 1:2] * value
        return carry

    lax.fori_loop(0, 16, step, 0, unroll=4)


def halo_kernel(ha, from_a, wall_bulk, pb, work):
    x, p = here()
    cxd = speed_x(p)
    cx = jnp.where(x % 2 == 0, -cxd, cxd)
    cy, cz = lane_speeds(p, 16)
    source = from_a[...]
    rows = bulk_rows(
        [source[NK + k : NK + k + 1] for k in range(8)],
        source[NK + 8 : NK + 9],
        cx,
        cx,
        [source[NK + 9 : NK + 10] * (courant * cxd)],
    )
    work[...] = to_columns(jnp.concatenate(rows, 0))

    def step(i, carry):
        at = pl.ds(pl.multiple_of(i * 16, 16), 16)
        k = columns(work[at, :], 0)
        pb[at, :] = relaxed(ha[at, :] + k[13] * wall_bulk[at, :], k, shared_part(k, cy, cz), 1)
        return carry

    lax.fori_loop(0, 16, step, 0, unroll=4)


def final_kernel(
    ca, cb, pb, ghost, hb, from_a, from_b, own, state, table, out, fields, oa, ob, work, stage, sems
):
    x, p = here()
    odd = x % 2
    cxd = speed_x(p)
    sign_a = jnp.where(odd == 0, 1.0, -1.0)
    cx_a, cx_b = sign_a * cxd, -sign_a * cxd
    cy, cz = lane_speeds(p, 16)
    weights = transport_weights(cxd, cy, cz)
    edge = jnp.where(jnp.logical_or(x == 0, x == 7), 1.0, 0.0)
    inner = 1.0 - edge
    ta, tb, st = from_a[...], from_b[...], state[...]
    m = [spread(own[k : k + 1, :] + ta[k : k + 1] + tb[k : k + 1]) for k in range(NK)]
    params, rate = relax_params(m, table[...])
    table8 = jnp.concatenate([v[:1] for v in params], 0)
    for y in range(16):
        stage[:, y, :] = table8[:, 16 * y : 16 * y + 16]
    copies = [pltpu.make_async_copy(stage, fields, sems.at[8])]
    copies[0].start()
    tb = jnp.where(edge > 0.0, st[:10], tb[NK : NK + 10])

    rows = bulk_rows([tb[k : k + 1] for k in range(8)], tb[8:9], cx_a, cx_b)
    rows += bulk_rows([v[:1] for v in params], rate[:1], cx_a, cx_b)
    work[...] = to_columns(jnp.concatenate(rows, 0))

    for chunk, (begin, end) in enumerate(((0, 5), (5, 10), (10, 14), (14, 16))):

        def second(i, carry):
            at = pl.ds(pl.multiple_of(i * 16, 16), 16)
            up = upwind_y(p, i)
            c = work[at, :]
            kb, k = columns(c, 0), columns(c, NCOL)
            part = shared_part(k, cy, cz)
            halo = relaxed(hb[at, :], kb, shared_part(kb, cy, cz), 0)
            read = transport_block(ca[at, :], ca[up, :], inner * halo + ghost[at, :], weights)
            oa[at, :] = relaxed(read, k, part, 0)
            read = transport_block(cb[at, :], cb[up, :], pb[at, :], weights)
            ob[at, :] = relaxed(read, k, part, 1)
            return carry

        lax.fori_loop(begin, end, second, 0, unroll=end - begin)
        at = pl.ds(16 * begin, 16 * (end - begin))
        for half, source, start in ((0, oa, 1 - odd), (1, ob, odd)):
            copy = pltpu.make_async_copy(
                source.at[at, :], out.at[at, pl.ds(half_start(start), HALF)], sems.at[2 * chunk + half]
            )
            copy.start()
            copies.append(copy)
    for copy in copies:
        copy.wait()


VMEM = pl.BlockSpec(memory_space=pltpu.VMEM)
ANY = pl.BlockSpec(memory_space=pltpu.HBM)
PLANE = (CELLS, HALF)


def call(kernel, outs, args, scratch=(), sems=0, loose_in=(), loose_out=(), cost=1_000_000, grant=16):
    scratches = [pltpu.VMEM(s, f32) for s in scratch]
    if sems:
        scratches.append(pltpu.SemaphoreType.DMA((sems,)))
    return pl.pallas_call(
        kernel,
        out_shape=[jax.ShapeDtypeStruct(s, f32) for s in outs],
        in_specs=[ANY if k in loose_in else VMEM for k in range(len(args))],
        out_specs=[ANY if k in loose_out else VMEM for k in range(len(outs))],
        scratch_shapes=scratches,
        cost_estimate=pl.CostEstimate(flops=cost, bytes_accessed=1 << 20, transcendentals=0),
        compiler_params=pltpu.CompilerParams(vmem_limit_bytes=grant << 20),
    )(*args)


PAIRS_A = [(i, i ^ 1) for i in range(8)]
PAIRS_B = [pair for i in (1, 3, 5) for pair in ((i, i + 1), (i + 1, i))]
SWAP = [(0, 1), (1, 0)]


def both_ways(pairs):
    return [pair for i, j in pairs for pair in ((i, j), (j, i))]


Z_ROUNDS = [
    ("zround1", both_ways([(0, 1), (2, 3), (4, 5), (6, 7)])),
    ("zround2", both_ways([(0, 2), (1, 3), (4, 6), (5, 7)])),
    ("zround3", both_ways([(0, 6), (1, 7), (2, 4), (3, 5)])),
]


def swap_planes(a, b):
    b = lax.ppermute(b, "space", PAIRS_B)
    a = lax.ppermute(a, "space", PAIRS_A)
    return a, b


def body(distribution, inflow, wall_temp, face_type):
    f = distribution.reshape(CELLS, 2 * HALF)
    fa, fb = call(split_kernel, [PLANE, PLANE], [f], sems=2, loose_in=(0,))
    ha, hb = swap_planes(fa, fb)
    temp = wall_temp.reshape(2, CELLS)
    kind = face_type.reshape(2, CELLS)
    table = jnp.asarray(TABLE)
    infl, wa, wb, pre, wall, wall_bulk, cols = call(
        setup_kernel,
        [PLANE, (ROWS, HALF), (ROWS, HALF), (ROWS, CELLS), (2 * NK * 8, CELLS), PLANE, (CELLS, 128)],
        [inflow.reshape(2, CELLS, 2 * HALF), fb, temp, kind, jnp.asarray(WALL_TABLES)],
        sems=1,
        loose_in=(0,),
    )
    rb, rows_b = call(read_b_kernel, [PLANE, (ROWS, CELLS)], [fb, ha, wb, pre])
    ra, keep, send = call(
        read_a_kernel, [PLANE, (HROWS, CELLS), (HROWS, CELLS)], [fa, hb, infl, cols, wa, rows_b]
    )
    part = keep + lax.ppermute(send, "core", SWAP)
    part = part + lax.ppermute(part, "ylo", SWAP)
    ga = lax.optimization_barrier((ra, part))[0]
    gb = rb
    for name, pairs in Z_ROUNDS:
        if name == "zround2":
            gb = lax.optimization_barrier((rb, part))[0]
        part = part + lax.ppermute(part, "z", pairs)
    ga, gb = swap_planes(ga, gb)
    other = lax.ppermute(part, "core", SWAP)
    send_a, send_b, own, state = call(
        cell_kernel,
        [(24, CELLS), (24, CELLS), (16, CELLS), (16, CELLS)],
        [part, other, wall, kind, table],
    )
    from_a, from_b = swap_planes(send_a, send_b)
    ca, cb, ghost = call(
        own_kernel, [PLANE] * 3, [ra, rb, state, wall_bulk, infl, cols], scratch=[(CELLS, 128)]
    )
    (pb,) = call(halo_kernel, [PLANE], [ga, from_a, wall_bulk], scratch=[(CELLS, 128)])
    out, fields = call(
        final_kernel,
        [(CELLS, 2 * HALF), (8, 16, 16)],
        [ca, cb, pb, ghost, gb, from_a, from_b, own, state, table],
        scratch=[PLANE] * 2 + [(CELLS, 128), (8, 16, 16)],
        sems=9,
        loose_out=(0, 1),
    )
    return out.reshape(1, 16, 16, 2 * HALF), fields[:, None]


def solution(mesh):
    split = Mesh(mesh.devices.reshape(8, 8, 2, 2), ("space", "z", "ylo", "core"))
    vel = ("z", "ylo", "core")
    in_specs = (P("space", None, None, vel), P(None, None, None, vel), P(), P())
    out_specs = (P("space", None, None, vel), P(None, "space", None, None))

    return jax.shard_map(body, mesh=split, in_specs=in_specs, out_specs=out_specs, check_vma=False)
```

```python
import jax
import jax.numpy as jnp
import numpy as np
from jax import lax
from jax.experimental import pallas as pl
from jax.experimental.pallas import tpu as pltpu
from jax.sharding import Mesh, PartitionSpec as P


NV = 32768
CELLS = 256
HALF = 512
NK = 13
ROWS = 96
HROWS = ROWS // 2
courant = 0.08
rate_field = 0.8
box_volume = 512.0
HIGHEST = lax.Precision.HIGHEST
f32 = jnp.float32

MOMENTS = [
    [(0, 0, 0)],
    [(1, 0, 0)],
    [(0, 1, 0)],
    [(0, 0, 1)],
    [(2, 0, 0)],
    [(0, 2, 0)],
    [(0, 0, 2)],
    [(1, 1, 0)],
    [(1, 0, 1)],
    [(0, 1, 1)],
    [(3, 0, 0), (1, 2, 0), (1, 0, 2)],
    [(2, 1, 0), (0, 3, 0), (0, 1, 2)],
    [(2, 0, 1), (0, 2, 1), (0, 0, 3)],
]


def axis_table(top):
    grid = (np.arange(32) + 0.5) * 0.25 - 4.0
    plus, minus = courant * np.maximum(grid, 0.0), courant * np.maximum(-grid, 0.0)
    table = np.zeros((24 * top, 96))
    for axis in range(3):
        for power in range(top):
            for d in range(7):
                row = grid**power
                if d == 1 + 2 * axis:
                    row = row * plus
                if d == 2 + 2 * axis:
                    row = row * minus
                table[8 * top * axis + 8 * power + d, 32 * axis : 32 * axis + 32] = row
    return table.astype(np.float32), plus, minus


def wall_tables():
    table, plus, minus = axis_table(4)
    walls = []
    for weight in (plus, minus):
        wall = table.copy()
        wall[:32, :32] *= weight
        walls.append(np.concatenate([table, wall]))
    return np.stack(walls).astype(np.float32)


TOP = 7


def two_parts(table):
    table = np.concatenate([table, np.zeros((-len(table) % 16, 96), np.float32)])
    high = table.astype(jnp.bfloat16)
    low = (table - high.astype(np.float32)).astype(jnp.bfloat16)
    return np.concatenate([high, low])


TABLE = two_parts(axis_table(TOP)[0])
WALL_TABLES = wall_tables()


def dot(a, b):
    return lax.dot_general(a, b, (((1,), (0,)), ((), ())), precision=HIGHEST, preferred_element_type=f32)


def dot_t(a, b):
    return lax.dot_general(a, b, (((1,), (1,)), ((), ())), precision=HIGHEST, preferred_element_type=f32)


def split(a):
    high = a.astype(jnp.bfloat16)
    return high, (a - high.astype(f32)).astype(jnp.bfloat16)


def dot_parts(parts, b, side):
    high, low = split(b)
    rows = parts.shape[0] // 2
    dims = (((1,), (side,)), ((), ()))
    first = lax.dot_general(parts, high, dims, preferred_element_type=f32)
    second = lax.dot_general(parts[:rows], low, dims, preferred_element_type=f32)
    return first[:rows] + (first[rows:] + second)


def tile4(a):
    return jnp.concatenate([a] * 4, 0)


def speed_grid():
    return (lax.broadcasted_iota(jnp.int32, (32, CELLS), 0).astype(f32) + 0.5) * 0.25 - 4.0


def lane_speeds(p, rows):
    lane = lax.broadcasted_iota(jnp.int32, (rows, HALF), 1)
    cy = ((lane // 32 + (p % 2) * 16).astype(f32) + 0.5) * 0.25 - 4.0
    cz = ((lane % 32).astype(f32) + 0.5) * 0.25 - 4.0
    return cy, cz


def speed_x(p):
    return ((p // 2).astype(f32) + 0.5) * 0.25


def to_columns(rows):
    pad = 128 - rows.shape[0]
    return jnp.transpose(jnp.concatenate([rows, jnp.zeros((pad, CELLS), f32)], 0))


def equilibrium_moments(params, table):
    n, ux, uy, uz, temp, qx, qy, qz = params
    inv = 1.0 / temp
    two_pi = 2.0 * np.pi * temp
    pref = n * box_volume / (two_pi * jnp.sqrt(two_pi))
    scale = inv * inv / (15.0 * n)
    grid = speed_grid()
    decay = tile4(-0.5 * inv)
    decays = []
    for u in (ux, uy, uz):
        w = grid - tile4(u)
        decays.append(jnp.exp(w * w * decay))
    sums = dot_parts(table, jnp.concatenate(decays, 0), 0)
    factors = []
    for axis, (u, q) in enumerate(((ux, qx), (uy, qy), (uz, qz))):
        kq = q * scale
        base = 8 * TOP * axis
        levels = [[sums[base + 8 * a : base + 8 * a + 8] for a in range(TOP)]]
        for _ in range(3):
            last = levels[-1]
            levels.append([last[a + 1] - u * last[a] for a in range(len(last) - 1)])
        powers = []
        for power in range(4):
            t0, t1, t2, t3 = [level[power] for level in levels]
            powers.append((t0, kq * t1, t2 * inv, kq * (t3 * inv - 5.0 * t1)))
        factors.append(powers)
    xs, ys, zs = factors
    pairs = {}

    def pair(ay, az):
        if (ay, az) not in pairs:
            y0, y1, y2, y3 = ys[ay]
            z0, z1, z2, z3 = zs[az]
            a = y0 * z0
            b = a + y3 * z0 + y0 * z3 + y1 * z2 + y2 * z1
            pairs[(ay, az)] = (a, b, y2 * z0 + y0 * z2, y1 * z0 + y0 * z1)
        return pairs[(ay, az)]

    out = []
    for terms in MOMENTS:
        total = 0.0
        for ax, ay, az in terms:
            x0, x1, x2, x3 = xs[ax]
            a, b, c, d = pair(ay, az)
            total = total + (x0 * b + x3 * a + x1 * c + x2 * d)
        out.append(pref * total)
    return out


def wall_moments(temp, tables):
    grid = speed_grid()
    g = jnp.exp(grid * grid * tile4(-0.5 / temp))
    sums = dot(tables, jnp.concatenate([g] * 3, 0))
    two_pi = 2.0 * np.pi * temp
    pref = box_volume / (two_pi * jnp.sqrt(two_pi))
    out = []
    for base in (0, 96):
        for terms in MOMENTS:
            total = 0.0
            for powers in terms:
                part = pref
                for axis in range(3):
                    row = base + 32 * axis + 8 * powers[axis]
                    part = part * sums[row : row + 8]
                total = total + part
            out.append(total)
    return out


def macro(m):
    m = [a * (1.0 / NV) for a in m]
    n = m[0]
    rn = 1.0 / n
    ux, uy, uz = m[1] * rn, m[2] * rn, m[3] * rn
    square = ux * ux + uy * uy + uz * uz
    energy = m[4] + m[5] + m[6]
    temp = (energy - n * square) * rn * (1.0 / 3.0)
    lift = 2.0 * n * square - energy
    qx = 0.5 * (m[10] + ux * lift) - (ux * m[4] + uy * m[7] + uz * m[8])
    qy = 0.5 * (m[11] + uy * lift) - (ux * m[7] + uy * m[5] + uz * m[9])
    qz = 0.5 * (m[12] + uz * lift) - (ux * m[8] + uy * m[9] + uz * m[6])
    rate = rate_field * n * jnp.exp(0.19 * jnp.log(temp))
    return (n, ux, uy, uz, temp, qx, qy, qz), rate


def spread(row):
    return jnp.broadcast_to(row, (8, CELLS))


def relax_params(m, table):
    params, rate = macro(m)
    for _ in range(2):
        s = [spread(a[:1]) for a in equilibrium_moments(params, table)]
        inv = 1.0 / (1.0 + rate)
        params, rate = macro([(a + rate * b) * inv for a, b in zip(m, s)])
    return params, rate


def here():
    x = lax.axis_index("space")
    p = lax.axis_index("z") * 4 + lax.axis_index("ylo") * 2 + lax.axis_index("core")
    return x, p


def half_start(index):
    return pl.multiple_of(index * HALF, HALF)


def split_kernel(f, fa, fb, sems):
    x, _ = here()
    odd = x % 2
    first = pltpu.make_async_copy(f.at[:, pl.ds(half_start(1 - odd), HALF)], fa, sems.at[0])
    second = pltpu.make_async_copy(f.at[:, pl.ds(half_start(odd), HALF)], fb, sems.at[1])
    first.start()
    second.start()
    first.wait()
    second.wait()


def setup_kernel(inflow, fb, temp_ref, type_ref, tables, infl, pa, pb, pre, wall, wall_bulk, cols, wa, wb, sems):
    x, p = here()
    odd = x % 2
    face = jnp.where(x >= 4, 1, 0)
    copy = pltpu.make_async_copy(inflow.at[face, :, pl.ds(half_start(1 - odd), HALF)], infl, sems.at[0])
    copy.start()
    cxd = speed_x(p)
    cy, cz = lane_speeds(p, 8)
    d = lax.broadcasted_iota(jnp.int32, (8, HALF), 0)
    yp, ym = courant * jnp.maximum(cy, 0.0), courant * jnp.maximum(-cy, 0.0)
    zp, zm = courant * jnp.maximum(cz, 0.0), courant * jnp.maximum(-cz, 0.0)
    sign_a = jnp.where(odd == 0, 1.0, -1.0)
    for w, sign in ((wa, sign_a), (wb, -sign_a)):
        cx = sign * cxd
        xp, xm = courant * jnp.maximum(cx, 0.0), courant * jnp.maximum(-cx, 0.0)
        plus = jnp.where(d == 0, 1.0, jnp.where(d == 1, xp, jnp.where(d == 3, yp, jnp.where(d == 5, zp, 0.0))))
        full = jnp.where(d == 2, xm, jnp.where(d == 4, ym, jnp.where(d == 6, zm, plus)))
        ypow = [1.0, cy, cy * cy, cy * cy * cy]
        zpow = [1.0, cz, cz * cz, cz * cz * cz]
        xpow = [1.0, cx, cx * cx, cx * cx * cx]
        phis = []
        for terms in MOMENTS:
            phi = 0.0
            for ax, ay, az in terms:
                phi = phi + xpow[ax] * (ypow[ay] * zpow[az])
            phis.append(phi)
        gaps = jnp.where(d == 2, xp, jnp.where(d == 4, yp, jnp.where(d == 6, zp, 0.0)))
        w[0:8, :] = plus * phis[0] + gaps * phis[3]
        w[8:16, :] = plus * phis[1] + jnp.where(d == 2, phis[3], 0.0)
        w[16:24, :] = plus * phis[2]
        for k in range(4, NK):
            w[8 * k - 8 : 8 * k, :] = full * phis[k]
    edge = jnp.where(jnp.logical_or(x == 0, x == 7), 1.0, 0.0)
    sub = lax.broadcasted_iota(jnp.int32, (8, CELLS), 0)
    temp = jnp.broadcast_to(temp_ref[pl.ds(face, 1), :], (8, CELLS))
    kind = jnp.broadcast_to(type_ref[pl.ds(face, 1), :], (8, CELLS))
    for k, value in enumerate(wall_moments(temp, tables[face])):
        wall[8 * k : 8 * k + 8, :] = value
    two_pi = 2.0 * np.pi * temp
    rows = jnp.where(sub == 0, jnp.where(kind == 1, edge, 0.0), 0.0)
    rows = jnp.where(sub == 1, jnp.where(kind == 2, edge, 0.0), rows)
    rows = jnp.where(sub == 2, -0.5 / temp, rows)
    rows = jnp.where(sub == 3, box_volume / (two_pi * jnp.sqrt(two_pi)), rows)
    cols[...] = to_columns(rows)
    cy16, cz16 = lane_speeds(p, 16)
    speed_sq = cy16 * cy16 + cz16 * cz16 + cxd * cxd

    def step(i, carry):
        at = pl.ds(pl.multiple_of(i * 16, 16), 16)
        c = cols[at, :]
        wall_bulk[at, :] = c[:, 3:4] * jnp.exp(speed_sq * c[:, 2:3])
        return carry

    lax.fori_loop(0, 16, step, 0, unroll=4)
    for w, parts in ((wa, pa), (wb, pb)):
        high, low = split(w[...])
        parts[:ROWS, :] = high
        parts[ROWS:, :] = low
    flux = dot_t(jnp.full((8, HALF), 1.0, f32), fb[...]) * (cxd * edge)
    copy.wait()
    in_rows = dot_t(wa[...], infl[...]) * (courant * cxd * edge)
    for group in range(ROWS // 8):
        value = jnp.where(sub == 7, spread(in_rows[8 * group : 8 * group + 1]), 0.0)
        if group == 1:
            value = jnp.where(sub == 6, spread(in_rows[10:11]), jnp.where(sub == 4, flux, value))
        pre[8 * group : 8 * group + 8, :] = value


def upwind_y(p, i):
    return pl.ds(pl.multiple_of(((i + jnp.where(p % 2 == 1, 15, 1)) % 16) * 16, 16), 16)


def transport_weights(cxd, cy, cz):
    abs_y, abs_z = courant * jnp.abs(cy), courant * jnp.abs(cz)
    return 1.0 - courant * cxd - abs_y - abs_z, courant * cxd, abs_y, abs_z, cz > 0.0


def transport_block(value, neighbour_y, plane, weights):
    centre, abs_x, abs_y, abs_z, forward = weights
    neighbour_z = jnp.where(forward, pltpu.roll(value, 1, 0), pltpu.roll(value, 15, 0))
    return value * centre + abs_x * plane + abs_y * neighbour_y + abs_z * neighbour_z


def read_b_kernel(fb, ha, wb, pre, rb, rows):
    _, p = here()
    weights = transport_weights(speed_x(p), *lane_speeds(p, 16))

    def step(i, carry):
        at = pl.ds(pl.multiple_of(i * 16, 16), 16)
        rb[at, :] = transport_block(fb[at, :], fb[upwind_y(p, i), :], ha[at, :], weights)
        return carry

    lax.fori_loop(0, 16, step, 0, unroll=4)
    rows[...] = pre[...] + dot_parts(wb[...], rb[...], 1)


def read_a_kernel(fa, hb, infl, cols, wa, rows_b, ra, keep, send):
    x, p = here()
    inner = jnp.where(jnp.logical_or(x == 0, x == 7), 0.0, 1.0)
    weights = transport_weights(speed_x(p), *lane_speeds(p, 16))

    def step(i, carry):
        at = pl.ds(pl.multiple_of(i * 16, 16), 16)
        c = cols[at, :]
        value = fa[at, :]
        plane = hb[at, :] * inner + infl[at, :] * c[:, 0:1] + c[:, 1:2] * value
        ra[at, :] = transport_block(value, fa[upwind_y(p, i), :], plane, weights)
        return carry

    lax.fori_loop(0, 16, step, 0, unroll=4)
    rows = rows_b[...] + dot_parts(wa[...], ra[...], 1)
    north = p % 2 == 1
    top, bottom = rows[:HROWS], rows[HROWS:]
    keep[...] = jnp.where(north, bottom, top)
    send[...] = jnp.where(north, top, bottom)


def unpack_rows(groups, sub):
    first, second = groups[0], groups[1]
    plain = [groups[0][:1], groups[1][:1], groups[2][:1], groups[1][2:3]] + [g[:1] for g in groups[3:]]
    odd = jnp.logical_or(sub == 1, jnp.logical_or(sub == 3, sub == 5))
    even = jnp.logical_or(sub == 2, jnp.logical_or(sub == 4, sub == 6))
    products = [(1, 2, 3), (4, 7, 8), (7, 5, 9), (8, 9, 6)]

    def less(plus, k):
        ix, iy, iz = products[k]
        change = jnp.where(sub == 2, spread(plain[ix]), jnp.where(sub == 4, spread(plain[iy]), spread(plain[iz])))
        return plus - courant * change

    out = []
    for k in range(3):
        out.append(jnp.where(even, less(pltpu.roll(groups[k], 1, 0), k), groups[k]))
    rest = jnp.where(sub == 0, spread(second[2:3]), spread(second[6:7]))
    out.append(jnp.where(odd, pltpu.roll(first, 7, 0), jnp.where(even, less(first, 3), rest)))
    return out + list(groups[3:]), second[4:5]


def cell_kernel(mine, other, wall, type_ref, table, send_a, send_b, own, state):
    x, p = here()
    upper = x == 7
    odd = x % 2 == 1
    face = jnp.where(x >= 4, 1, 0)
    edge = jnp.where(jnp.logical_or(x == 0, upper), 1.0, 0.0)
    north = p % 2 == 1
    a, b = mine[...], other[...]
    rows = jnp.concatenate([jnp.where(north, b, a), jnp.where(north, a, b)], 0)
    sub = lax.broadcasted_iota(jnp.int32, (8, CELLS), 0)
    m, leaving = unpack_rows([rows[8 * k : 8 * k + 8] for k in range(ROWS // 8)], sub)
    plain = [wall[8 * k : 8 * k + 8, :] for k in range(NK)]
    kind = jnp.broadcast_to(type_ref[pl.ds(face, 1), :], (8, CELLS))
    is_wall = jnp.where(kind == 0, edge, 0.0)
    is_in = jnp.where(kind == 1, edge, 0.0)
    is_out = jnp.where(kind == 2, edge, 0.0)

    def first(v):
        return jnp.where(odd, v[2:3], v[1:2])

    def second(v):
        return jnp.where(odd, v[1:2], v[2:3])

    entering = spread(first(plain[0])) * (1.0 / courant)
    amp = is_wall * spread(leaving) / entering
    inflow = [v[7:8] for v in m]
    m = [v + amp * wall[8 * (NK + k) : 8 * (NK + k) + 8, :] for k, v in enumerate(m)]
    params, rate = relax_params([spread(v[:1]) for v in m], table[...])
    s = equilibrium_moments(params, table[...])
    inv = 1.0 / (1.0 + rate)
    m = [(v + rate * w) * inv for v, w in zip(m, s)]
    amp2 = is_wall * spread(second(m[0])) * (1.0 / courant) / entering
    lane = lax.broadcasted_iota(jnp.int32, (8, CELLS), 1)
    low, high = lane % 16 == 0, lane % 16 == 15
    for k in range(NK):
        v = m[k]
        z_up = jnp.where(low, pltpu.roll(v, CELLS - 15, 1), pltpu.roll(v, 1, 1))
        z_down = jnp.where(high, pltpu.roll(v, 15, 1), pltpu.roll(v, CELLS - 1, 1))
        total = jnp.where(sub == 0, v, jnp.where(sub == 7, 0.0, -v))
        total = total + jnp.where(sub == 3, pltpu.roll(v, 16, 1), 0.0)
        total = total + jnp.where(sub == 4, pltpu.roll(v, CELLS - 16, 1), 0.0)
        total = total + jnp.where(sub == 5, z_up, 0.0) + jnp.where(sub == 6, z_down, 0.0)
        va = first(v)
        ghost = amp2[:1] * first(plain[k]) + is_in[:1] * inflow[k] + is_out[:1] * va
        own[k : k + 1, :] = jnp.sum(total, 0, keepdims=True) + ghost
        send_a[k : k + 1, :] = va
        send_b[k : k + 1, :] = second(v)
    own[NK:16, :] = jnp.zeros((3, CELLS), f32)
    extra = list(params) + [rate, amp]
    for k, v in enumerate(extra):
        send_a[NK + k : NK + k + 1, :] = v[:1]
        send_b[NK + k : NK + k + 1, :] = v[:1]
        state[k : k + 1, :] = v[:1]
    send_a[23:24, :] = jnp.zeros((1, CELLS), f32)
    send_b[23:24, :] = jnp.zeros((1, CELLS), f32)
    state[10:11, :] = amp2[:1]
    state[11:16, :] = jnp.zeros((5, CELLS), f32)


NCOL = 16


def bulk_rows(params, rate, cx_a, cx_b, extra=()):
    n, ux, uy, uz, temp, qx, qy, qz = params
    inv = 1.0 / temp
    two_pi = 2.0 * np.pi * temp
    share = 1.0 / (1.0 + rate)
    scale = inv * inv / (15.0 * n)
    pref = rate * share * n * box_volume / (two_pi * jnp.sqrt(two_pi))
    rows = [uy, uz, -0.5 * inv, inv, qy * scale, qz * scale, share]
    for cx in (cx_a, cx_b):
        w = cx - ux
        square = w * w
        rows += [pref * jnp.exp(-0.5 * inv * square), qx * scale * w, square * inv]
    rows += list(extra)
    return rows + [jnp.zeros((1, CELLS), f32)] * (NCOL - len(rows))


def columns(c, base):
    return [c[:, base + j : base + j + 1] for j in range(NCOL)]


def shared_part(k, cy, cz):
    wy = cy - k[0]
    wz = cz - k[1]
    square = wy * wy + wz * wz
    return jnp.exp(square * k[2]), square * k[3] - 5.0, wy * k[4] + wz * k[5]


def relaxed(value, k, part, half):
    decay, square, heat = part
    pref, heat_x, square_x = k[7 + 3 * half : 10 + 3 * half]
    return value * k[6] + (decay * pref) * (1.0 + (heat + heat_x) * (square + square_x))


def own_kernel(ra, rb, state, wall_bulk, infl, cols, ca, cb, ghost, work):
    x, p = here()
    cxd = speed_x(p)
    sign_a = jnp.where(x % 2 == 0, 1.0, -1.0)
    cy, cz = lane_speeds(p, 16)
    st = state[...]
    rows = bulk_rows(
        [st[k : k + 1] for k in range(8)], st[8:9], sign_a * cxd, -sign_a * cxd, [st[9:10] * (courant * cxd), st[10:11]]
    )
    work[...] = to_columns(jnp.concatenate(rows, 0))

    def step(i, carry):
        at = pl.ds(pl.multiple_of(i * 16, 16), 16)
        k = columns(work[at, :], 0)
        part = shared_part(k, cy, cz)
        face = cols[at, :]
        w = wall_bulk[at, :]
        value = relaxed(ra[at, :] + k[13] * w, k, part, 0)
        ca[at, :] = value
        cb[at, :] = relaxed(rb[at, :], k, part, 1)
        ghost[at, :] = infl[at, :] * face[:, 0:1] + k[14] * w + face[:, 1:2] * value
        return carry

    lax.fori_loop(0, 16, step, 0, unroll=4)


def halo_kernel(ha, from_a, wall_bulk, pb, work):
    x, p = here()
    cxd = speed_x(p)
    cx = jnp.where(x % 2 == 0, -cxd, cxd)
    cy, cz = lane_speeds(p, 16)
    source = from_a[...]
    rows = bulk_rows(
        [source[NK + k : NK + k + 1] for k in range(8)],
        source[NK + 8 : NK + 9],
        cx,
        cx,
        [source[NK + 9 : NK + 10] * (courant * cxd)],
    )
    work[...] = to_columns(jnp.concatenate(rows, 0))

    def step(i, carry):
        at = pl.ds(pl.multiple_of(i * 16, 16), 16)
        k = columns(work[at, :], 0)
        pb[at, :] = relaxed(ha[at, :] + k[13] * wall_bulk[at, :], k, shared_part(k, cy, cz), 1)
        return carry

    lax.fori_loop(0, 16, step, 0, unroll=4)


def final_kernel(
    ca, cb, pb, ghost, hb, from_a, from_b, own, state, table, out, fields, oa, ob, work, stage, sems
):
    x, p = here()
    odd = x % 2
    cxd = speed_x(p)
    sign_a = jnp.where(odd == 0, 1.0, -1.0)
    cx_a, cx_b = sign_a * cxd, -sign_a * cxd
    cy, cz = lane_speeds(p, 16)
    weights = transport_weights(cxd, cy, cz)
    edge = jnp.where(jnp.logical_or(x == 0, x == 7), 1.0, 0.0)
    inner = 1.0 - edge
    ta, tb, st = from_a[...], from_b[...], state[...]
    m = [spread(own[k : k + 1, :] + ta[k : k + 1] + tb[k : k + 1]) for k in range(NK)]
    params, rate = relax_params(m, table[...])
    table8 = jnp.concatenate([v[:1] for v in params], 0)
    for y in range(16):
        stage[:, y, :] = table8[:, 16 * y : 16 * y + 16]
    copies = [pltpu.make_async_copy(stage, fields, sems.at[8])]
    copies[0].start()
    tb = jnp.where(edge > 0.0, st[:10], tb[NK : NK + 10])

    rows = bulk_rows([tb[k : k + 1] for k in range(8)], tb[8:9], cx_a, cx_b)
    rows += bulk_rows([v[:1] for v in params], rate[:1], cx_a, cx_b)
    work[...] = to_columns(jnp.concatenate(rows, 0))

    for chunk, (begin, end) in enumerate(((0, 5), (5, 10), (10, 14), (14, 16))):

        def second(i, carry):
            at = pl.ds(pl.multiple_of(i * 16, 16), 16)
            up = upwind_y(p, i)
            c = work[at, :]
            kb, k = columns(c, 0), columns(c, NCOL)
            part = shared_part(k, cy, cz)
            halo = relaxed(hb[at, :], kb, shared_part(kb, cy, cz), 0)
            read = transport_block(ca[at, :], ca[up, :], inner * halo + ghost[at, :], weights)
            oa[at, :] = relaxed(read, k, part, 0)
            read = transport_block(cb[at, :], cb[up, :], pb[at, :], weights)
            ob[at, :] = relaxed(read, k, part, 1)
            return carry

        lax.fori_loop(begin, end, second, 0, unroll=end - begin)
        at = pl.ds(16 * begin, 16 * (end - begin))
        for half, source, start in ((0, oa, 1 - odd), (1, ob, odd)):
            copy = pltpu.make_async_copy(
                source.at[at, :], out.at[at, pl.ds(half_start(start), HALF)], sems.at[2 * chunk + half]
            )
            copy.start()
            copies.append(copy)
    for copy in copies:
        copy.wait()


VMEM = pl.BlockSpec(memory_space=pltpu.VMEM)
ANY = pl.BlockSpec(memory_space=pltpu.HBM)
PLANE = (CELLS, HALF)
PARTS = (2 * ROWS, HALF)


def call(kernel, outs, args, scratch=(), sems=0, loose_in=(), loose_out=(), cost=1_000_000, grant=16):
    scratches = [pltpu.VMEM(s, f32) for s in scratch]
    if sems:
        scratches.append(pltpu.SemaphoreType.DMA((sems,)))
    return pl.pallas_call(
        kernel,
        out_shape=[jax.ShapeDtypeStruct(s, jnp.bfloat16 if s is PARTS else f32) for s in outs],
        in_specs=[ANY if k in loose_in else VMEM for k in range(len(args))],
        out_specs=[ANY if k in loose_out else VMEM for k in range(len(outs))],
        scratch_shapes=scratches,
        cost_estimate=pl.CostEstimate(flops=cost, bytes_accessed=1 << 20, transcendentals=0),
        compiler_params=pltpu.CompilerParams(vmem_limit_bytes=grant << 20),
    )(*args)


PAIRS_A = [(i, i ^ 1) for i in range(8)]
PAIRS_B = [pair for i in (1, 3, 5) for pair in ((i, i + 1), (i + 1, i))]
SWAP = [(0, 1), (1, 0)]


def both_ways(pairs):
    return [pair for i, j in pairs for pair in ((i, j), (j, i))]


Z_ROUNDS = [
    ("zround1", both_ways([(0, 1), (2, 3), (4, 5), (6, 7)])),
    ("zround2", both_ways([(0, 2), (1, 3), (4, 6), (5, 7)])),
    ("zround3", both_ways([(0, 6), (1, 7), (2, 4), (3, 5)])),
]


def swap_planes(a, b):
    b = lax.ppermute(b, "space", PAIRS_B)
    a = lax.ppermute(a, "space", PAIRS_A)
    return a, b


def body(distribution, inflow, wall_temp, face_type):
    f = distribution.reshape(CELLS, 2 * HALF)
    fa, fb = call(split_kernel, [PLANE, PLANE], [f], sems=2, loose_in=(0,))
    ha, hb = swap_planes(fa, fb)
    temp = wall_temp.reshape(2, CELLS)
    kind = face_type.reshape(2, CELLS)
    table = jnp.asarray(TABLE)
    infl, wa, wb, pre, wall, wall_bulk, cols = call(
        setup_kernel,
        [PLANE, PARTS, PARTS, (ROWS, CELLS), (2 * NK * 8, CELLS), PLANE, (CELLS, 128)],
        [inflow.reshape(2, CELLS, 2 * HALF), fb, temp, kind, jnp.asarray(WALL_TABLES)],
        scratch=[(ROWS, HALF)] * 2,
        sems=1,
        loose_in=(0,),
    )
    rb, rows_b = call(read_b_kernel, [PLANE, (ROWS, CELLS)], [fb, ha, wb, pre])
    ra, keep, send = call(
        read_a_kernel, [PLANE, (HROWS, CELLS), (HROWS, CELLS)], [fa, hb, infl, cols, wa, rows_b]
    )
    part = keep + lax.ppermute(send, "core", SWAP)
    part = part + lax.ppermute(part, "ylo", SWAP)
    ga = lax.optimization_barrier((ra, part))[0]
    gb = rb
    for name, pairs in Z_ROUNDS:
        if name == "zround2":
            gb = lax.optimization_barrier((rb, part))[0]
        part = part + lax.ppermute(part, "z", pairs)
    ga, gb = swap_planes(ga, gb)
    other = lax.ppermute(part, "core", SWAP)
    send_a, send_b, own, state = call(
        cell_kernel,
        [(24, CELLS), (24, CELLS), (16, CELLS), (16, CELLS)],
        [part, other, wall, kind, table],
    )
    from_a, from_b = swap_planes(send_a, send_b)
    ca, cb, ghost = call(
        own_kernel, [PLANE] * 3, [ra, rb, state, wall_bulk, infl, cols], scratch=[(CELLS, 128)]
    )
    (pb,) = call(halo_kernel, [PLANE], [ga, from_a, wall_bulk], scratch=[(CELLS, 128)])
    out, fields = call(
        final_kernel,
        [(CELLS, 2 * HALF), (8, 16, 16)],
        [ca, cb, pb, ghost, gb, from_a, from_b, own, state, table],
        scratch=[PLANE] * 2 + [(CELLS, 128), (8, 16, 16)],
        sems=9,
        loose_out=(0, 1),
    )
    return out.reshape(1, 16, 16, 2 * HALF), fields[:, None]


def solution(mesh):
    split = Mesh(mesh.devices.reshape(8, 8, 2, 2), ("space", "z", "ylo", "core"))
    vel = ("z", "ylo", "core")
    in_specs = (P("space", None, None, vel), P(None, None, None, vel), P(), P())
    out_specs = (P("space", None, None, vel), P(None, "space", None, None))

    return jax.shard_map(body, mesh=split, in_specs=in_specs, out_specs=out_specs, check_vma=False)
```

```python
import jax
import jax.numpy as jnp
import numpy as np
from jax import lax
from jax.experimental import pallas as pl
from jax.experimental.pallas import tpu as pltpu
from jax.sharding import Mesh, PartitionSpec as P


NV = 32768
CELLS = 256
HALF = 512
NK = 13
ROWS = 96
HROWS = ROWS // 2
courant = 0.08
rate_field = 0.8
box_volume = 512.0
HIGHEST = lax.Precision.HIGHEST
f32 = jnp.float32

MOMENTS = [
    [(0, 0, 0)],
    [(1, 0, 0)],
    [(0, 1, 0)],
    [(0, 0, 1)],
    [(2, 0, 0)],
    [(0, 2, 0)],
    [(0, 0, 2)],
    [(1, 1, 0)],
    [(1, 0, 1)],
    [(0, 1, 1)],
    [(3, 0, 0), (1, 2, 0), (1, 0, 2)],
    [(2, 1, 0), (0, 3, 0), (0, 1, 2)],
    [(2, 0, 1), (0, 2, 1), (0, 0, 3)],
]


def axis_table(top):
    grid = (np.arange(32) + 0.5) * 0.25 - 4.0
    plus, minus = courant * np.maximum(grid, 0.0), courant * np.maximum(-grid, 0.0)
    table = np.zeros((24 * top, 96))
    for axis in range(3):
        for power in range(top):
            for d in range(7):
                row = grid**power
                if d == 1 + 2 * axis:
                    row = row * plus
                if d == 2 + 2 * axis:
                    row = row * minus
                table[8 * top * axis + 8 * power + d, 32 * axis : 32 * axis + 32] = row
    return table.astype(np.float32), plus, minus


def wall_tables():
    table, plus, minus = axis_table(4)
    walls = []
    for weight in (plus, minus):
        wall = table.copy()
        wall[:32, :32] *= weight
        walls.append(np.concatenate([table, wall]))
    return np.stack(walls).astype(np.float32)


TOP = 5


def two_parts(table):
    table = np.concatenate([table, np.zeros((-len(table) % 16, 96), np.float32)])
    high = table.astype(jnp.bfloat16)
    low = (table - high.astype(np.float32)).astype(jnp.bfloat16)
    return np.concatenate([high, low])


TABLE = two_parts(axis_table(TOP)[0])
WALL_TABLES = wall_tables()


def dot(a, b):
    return lax.dot_general(a, b, (((1,), (0,)), ((), ())), precision=HIGHEST, preferred_element_type=f32)


def dot_t(a, b):
    return lax.dot_general(a, b, (((1,), (1,)), ((), ())), precision=HIGHEST, preferred_element_type=f32)


def split(a):
    high = a.astype(jnp.bfloat16)
    return high, (a - high.astype(f32)).astype(jnp.bfloat16)


def dot_parts(parts, b, side):
    high, low = split(b)
    rows = parts.shape[0] // 2
    dims = (((1,), (side,)), ((), ()))
    first = lax.dot_general(parts, high, dims, preferred_element_type=f32)
    second = lax.dot_general(parts, low, dims, preferred_element_type=f32)
    return first[:rows] + (first[rows:] + second[:rows] + second[rows:])


def tile4(a):
    return jnp.concatenate([a] * 4, 0)


def speed_grid():
    return (lax.broadcasted_iota(jnp.int32, (32, CELLS), 0).astype(f32) + 0.5) * 0.25 - 4.0


def lane_speeds(p, rows):
    lane = lax.broadcasted_iota(jnp.int32, (rows, HALF), 1)
    cy = ((lane // 32 + (p % 2) * 16).astype(f32) + 0.5) * 0.25 - 4.0
    cz = ((lane % 32).astype(f32) + 0.5) * 0.25 - 4.0
    return cy, cz


def speed_x(p):
    return ((p // 2).astype(f32) + 0.5) * 0.25


def to_columns(rows):
    pad = 128 - rows.shape[0]
    return jnp.transpose(jnp.concatenate([rows, jnp.zeros((pad, CELLS), f32)], 0))


def equilibrium_moments(params, table):
    n, ux, uy, uz, temp, qx, qy, qz = params
    inv = 1.0 / temp
    two_pi = 2.0 * np.pi * temp
    pref = n * box_volume / (two_pi * jnp.sqrt(two_pi))
    scale = inv * inv / (15.0 * n)
    grid = speed_grid()
    decay = tile4(-0.5 * inv)
    columns = []
    for u in (ux, uy, uz):
        w = grid - tile4(u)
        square = w * w
        g = jnp.exp(square * decay)
        columns.append(jnp.concatenate([g, g * square], 1))
    sums = dot_parts(table, jnp.concatenate(columns, 0), 0)
    factors = []
    for axis, (u, q) in enumerate(((ux, qx), (uy, qy), (uz, qz))):
        kq = q * scale
        starts = [8 * (TOP * axis + power) for power in range(TOP)]
        even0 = [sums[row : row + 8, :CELLS] for row in starts]
        even2 = [sums[row : row + 8, CELLS:] for row in starts]
        powers = []
        for power in range(4):
            t0, t2 = even0[power], even2[power]
            t1 = even0[power + 1] - u * t0
            t3 = even2[power + 1] - u * t2
            powers.append((t0, kq * t1, t2 * inv, kq * (t3 * inv - 5.0 * t1)))
        factors.append(powers)
    xs, ys, zs = factors
    pairs = {}

    def pair(ay, az):
        if (ay, az) not in pairs:
            y0, y1, y2, y3 = ys[ay]
            z0, z1, z2, z3 = zs[az]
            a = y0 * z0
            b = a + y3 * z0 + y0 * z3 + y1 * z2 + y2 * z1
            pairs[(ay, az)] = (a, b, y2 * z0 + y0 * z2, y1 * z0 + y0 * z1)
        return pairs[(ay, az)]

    out = []
    for terms in MOMENTS:
        total = 0.0
        for ax, ay, az in terms:
            x0, x1, x2, x3 = xs[ax]
            a, b, c, d = pair(ay, az)
            total = total + (x0 * b + x3 * a + x1 * c + x2 * d)
        out.append(pref * total)
    return out


def wall_moments(temp, tables):
    grid = speed_grid()
    g = jnp.exp(grid * grid * tile4(-0.5 / temp))
    sums = dot(tables, jnp.concatenate([g] * 3, 0))
    two_pi = 2.0 * np.pi * temp
    pref = box_volume / (two_pi * jnp.sqrt(two_pi))
    out = []
    for base in (0, 96):
        for terms in MOMENTS:
            total = 0.0
            for powers in terms:
                part = pref
                for axis in range(3):
                    row = base + 32 * axis + 8 * powers[axis]
                    part = part * sums[row : row + 8]
                total = total + part
            out.append(total)
    return out


def macro(m):
    m = [a * (1.0 / NV) for a in m]
    n = m[0]
    rn = 1.0 / n
    ux, uy, uz = m[1] * rn, m[2] * rn, m[3] * rn
    square = ux * ux + uy * uy + uz * uz
    energy = m[4] + m[5] + m[6]
    temp = (energy - n * square) * rn * (1.0 / 3.0)
    lift = 2.0 * n * square - energy
    qx = 0.5 * (m[10] + ux * lift) - (ux * m[4] + uy * m[7] + uz * m[8])
    qy = 0.5 * (m[11] + uy * lift) - (ux * m[7] + uy * m[5] + uz * m[9])
    qz = 0.5 * (m[12] + uz * lift) - (ux * m[8] + uy * m[9] + uz * m[6])
    rate = rate_field * n * jnp.exp(0.19 * jnp.log(temp))
    return (n, ux, uy, uz, temp, qx, qy, qz), rate


def spread(row):
    return jnp.broadcast_to(row, (8, CELLS))


def relax_params(m, table):
    params, rate = macro(m)
    for _ in range(2):
        s = [spread(a[:1]) for a in equilibrium_moments(params, table)]
        inv = 1.0 / (1.0 + rate)
        params, rate = macro([(a + rate * b) * inv for a, b in zip(m, s)])
    return params, rate


def here():
    x = lax.axis_index("space")
    p = lax.axis_index("z") * 4 + lax.axis_index("ylo") * 2 + lax.axis_index("core")
    return x, p


def half_start(index):
    return pl.multiple_of(index * HALF, HALF)


def split_kernel(f, fa, fb, sems):
    x, _ = here()
    odd = x % 2
    first = pltpu.make_async_copy(f.at[:, pl.ds(half_start(1 - odd), HALF)], fa, sems.at[0])
    second = pltpu.make_async_copy(f.at[:, pl.ds(half_start(odd), HALF)], fb, sems.at[1])
    first.start()
    second.start()
    first.wait()
    second.wait()


def setup_kernel(inflow, fb, temp_ref, type_ref, tables, infl, pa, pb, pre, wall, wall_bulk, cols, wa, wb, sems):
    x, p = here()
    odd = x % 2
    face = jnp.where(x >= 4, 1, 0)
    copy = pltpu.make_async_copy(inflow.at[face, :, pl.ds(half_start(1 - odd), HALF)], infl, sems.at[0])
    copy.start()
    cxd = speed_x(p)
    cy, cz = lane_speeds(p, 8)
    d = lax.broadcasted_iota(jnp.int32, (8, HALF), 0)
    yp, ym = courant * jnp.maximum(cy, 0.0), courant * jnp.maximum(-cy, 0.0)
    zp, zm = courant * jnp.maximum(cz, 0.0), courant * jnp.maximum(-cz, 0.0)
    sign_a = jnp.where(odd == 0, 1.0, -1.0)
    for w, sign in ((wa, sign_a), (wb, -sign_a)):
        cx = sign * cxd
        xp, xm = courant * jnp.maximum(cx, 0.0), courant * jnp.maximum(-cx, 0.0)
        plus = jnp.where(d == 0, 1.0, jnp.where(d == 1, xp, jnp.where(d == 3, yp, jnp.where(d == 5, zp, 0.0))))
        full = jnp.where(d == 2, xm, jnp.where(d == 4, ym, jnp.where(d == 6, zm, plus)))
        ypow = [1.0, cy, cy * cy, cy * cy * cy]
        zpow = [1.0, cz, cz * cz, cz * cz * cz]
        xpow = [1.0, cx, cx * cx, cx * cx * cx]
        phis = []
        for terms in MOMENTS:
            phi = 0.0
            for ax, ay, az in terms:
                phi = phi + xpow[ax] * (ypow[ay] * zpow[az])
            phis.append(phi)
        gaps = jnp.where(d == 2, xp, jnp.where(d == 4, yp, jnp.where(d == 6, zp, 0.0)))
        w[0:8, :] = plus * phis[0] + gaps * phis[3]
        w[8:16, :] = plus * phis[1] + jnp.where(d == 2, phis[3], 0.0)
        w[16:24, :] = plus * phis[2]
        for k in range(4, NK):
            w[8 * k - 8 : 8 * k, :] = full * phis[k]
    edge = jnp.where(jnp.logical_or(x == 0, x == 7), 1.0, 0.0)
    sub = lax.broadcasted_iota(jnp.int32, (8, CELLS), 0)
    temp = jnp.broadcast_to(temp_ref[pl.ds(face, 1), :], (8, CELLS))
    kind = jnp.broadcast_to(type_ref[pl.ds(face, 1), :], (8, CELLS))
    for k, value in enumerate(wall_moments(temp, tables[face])):
        wall[8 * k : 8 * k + 8, :] = value
    two_pi = 2.0 * np.pi * temp
    rows = jnp.where(sub == 0, jnp.where(kind == 1, edge, 0.0), 0.0)
    rows = jnp.where(sub == 1, jnp.where(kind == 2, edge, 0.0), rows)
    rows = jnp.where(sub == 2, -0.5 / temp, rows)
    rows = jnp.where(sub == 3, box_volume / (two_pi * jnp.sqrt(two_pi)), rows)
    cols[...] = to_columns(rows)
    cy16, cz16 = lane_speeds(p, 16)
    speed_sq = cy16 * cy16 + cz16 * cz16 + cxd * cxd

    def step(i, carry):
        at = pl.ds(pl.multiple_of(i * 16, 16), 16)
        c = cols[at, :]
        wall_bulk[at, :] = c[:, 3:4] * jnp.exp(speed_sq * c[:, 2:3])
        return carry

    lax.fori_loop(0, 16, step, 0, unroll=4)
    for w, parts in ((wa, pa), (wb, pb)):
        high, low = split(w[...])
        parts[:ROWS, :] = high
        parts[ROWS:, :] = low
    flux = dot_t(jnp.full((8, HALF), 1.0, f32), fb[...]) * (cxd * edge)
    copy.wait()
    in_rows = dot_t(wa[...], infl[...]) * (courant * cxd * edge)
    for group in range(ROWS // 8):
        value = jnp.where(sub == 7, spread(in_rows[8 * group : 8 * group + 1]), 0.0)
        if group == 1:
            value = jnp.where(sub == 6, spread(in_rows[10:11]), jnp.where(sub == 4, flux, value))
        pre[8 * group : 8 * group + 8, :] = value


def upwind_y(p, i):
    return pl.ds(pl.multiple_of(((i + jnp.where(p % 2 == 1, 15, 1)) % 16) * 16, 16), 16)


def transport_weights(cxd, cy, cz):
    abs_y, abs_z = courant * jnp.abs(cy), courant * jnp.abs(cz)
    return 1.0 - courant * cxd - abs_y - abs_z, courant * cxd, abs_y, abs_z, cz > 0.0


def transport_block(value, neighbour_y, plane, weights):
    centre, abs_x, abs_y, abs_z, forward = weights
    neighbour_z = jnp.where(forward, pltpu.roll(value, 1, 0), pltpu.roll(value, 15, 0))
    return value * centre + abs_x * plane + abs_y * neighbour_y + abs_z * neighbour_z


def read_b_kernel(fb, ha, wb, pre, rb, rows):
    _, p = here()
    weights = transport_weights(speed_x(p), *lane_speeds(p, 16))

    def step(i, carry):
        at = pl.ds(pl.multiple_of(i * 16, 16), 16)
        rb[at, :] = transport_block(fb[at, :], fb[upwind_y(p, i), :], ha[at, :], weights)
        return carry

    lax.fori_loop(0, 16, step, 0, unroll=4)
    rows[...] = pre[...] + dot_parts(wb[...], rb[...], 1)


def read_a_kernel(fa, hb, infl, cols, wa, rows_b, ra, keep, send):
    x, p = here()
    inner = jnp.where(jnp.logical_or(x == 0, x == 7), 0.0, 1.0)
    weights = transport_weights(speed_x(p), *lane_speeds(p, 16))

    def step(i, carry):
        at = pl.ds(pl.multiple_of(i * 16, 16), 16)
        c = cols[at, :]
        value = fa[at, :]
        plane = hb[at, :] * inner + infl[at, :] * c[:, 0:1] + c[:, 1:2] * value
        ra[at, :] = transport_block(value, fa[upwind_y(p, i), :], plane, weights)
        return carry

    lax.fori_loop(0, 16, step, 0, unroll=4)
    rows = rows_b[...] + dot_parts(wa[...], ra[...], 1)
    north = p % 2 == 1
    top, bottom = rows[:HROWS], rows[HROWS:]
    keep[...] = jnp.where(north, bottom, top)
    send[...] = jnp.where(north, top, bottom)


def unpack_rows(groups, sub):
    first, second = groups[0], groups[1]
    plain = [groups[0][:1], groups[1][:1], groups[2][:1], groups[1][2:3]] + [g[:1] for g in groups[3:]]
    odd = jnp.logical_or(sub == 1, jnp.logical_or(sub == 3, sub == 5))
    even = jnp.logical_or(sub == 2, jnp.logical_or(sub == 4, sub == 6))
    products = [(1, 2, 3), (4, 7, 8), (7, 5, 9), (8, 9, 6)]

    def less(plus, k):
        ix, iy, iz = products[k]
        change = jnp.where(sub == 2, spread(plain[ix]), jnp.where(sub == 4, spread(plain[iy]), spread(plain[iz])))
        return plus - courant * change

    out = []
    for k in range(3):
        out.append(jnp.where(even, less(pltpu.roll(groups[k], 1, 0), k), groups[k]))
    rest = jnp.where(sub == 0, spread(second[2:3]), spread(second[6:7]))
    out.append(jnp.where(odd, pltpu.roll(first, 7, 0), jnp.where(even, less(first, 3), rest)))
    return out + list(groups[3:]), second[4:5]


def cell_kernel(mine, other, wall, type_ref, table, send_a, send_b, own, state):
    x, p = here()
    upper = x == 7
    odd = x % 2 == 1
    face = jnp.where(x >= 4, 1, 0)
    edge = jnp.where(jnp.logical_or(x == 0, upper), 1.0, 0.0)
    north = p % 2 == 1
    a, b = mine[...], other[...]
    rows = jnp.concatenate([jnp.where(north, b, a), jnp.where(north, a, b)], 0)
    sub = lax.broadcasted_iota(jnp.int32, (8, CELLS), 0)
    m, leaving = unpack_rows([rows[8 * k : 8 * k + 8] for k in range(ROWS // 8)], sub)
    plain = [wall[8 * k : 8 * k + 8, :] for k in range(NK)]
    kind = jnp.broadcast_to(type_ref[pl.ds(face, 1), :], (8, CELLS))
    is_wall = jnp.where(kind == 0, edge, 0.0)
    is_in = jnp.where(kind == 1, edge, 0.0)
    is_out = jnp.where(kind == 2, edge, 0.0)

    def first(v):
        return jnp.where(odd, v[2:3], v[1:2])

    def second(v):
        return jnp.where(odd, v[1:2], v[2:3])

    entering = spread(first(plain[0])) * (1.0 / courant)
    amp = is_wall * spread(leaving) / entering
    inflow = [v[7:8] for v in m]
    m = [v + amp * wall[8 * (NK + k) : 8 * (NK + k) + 8, :] for k, v in enumerate(m)]
    params, rate = relax_params([spread(v[:1]) for v in m], table[...])
    s = equilibrium_moments(params, table[...])
    inv = 1.0 / (1.0 + rate)
    m = [(v + rate * w) * inv for v, w in zip(m, s)]
    amp2 = is_wall * spread(second(m[0])) * (1.0 / courant) / entering
    lane = lax.broadcasted_iota(jnp.int32, (8, CELLS), 1)
    low, high = lane % 16 == 0, lane % 16 == 15
    for k in range(NK):
        v = m[k]
        z_up = jnp.where(low, pltpu.roll(v, CELLS - 15, 1), pltpu.roll(v, 1, 1))
        z_down = jnp.where(high, pltpu.roll(v, 15, 1), pltpu.roll(v, CELLS - 1, 1))
        total = jnp.where(sub == 0, v, jnp.where(sub == 7, 0.0, -v))
        total = total + jnp.where(sub == 3, pltpu.roll(v, 16, 1), 0.0)
        total = total + jnp.where(sub == 4, pltpu.roll(v, CELLS - 16, 1), 0.0)
        total = total + jnp.where(sub == 5, z_up, 0.0) + jnp.where(sub == 6, z_down, 0.0)
        va = first(v)
        ghost = amp2[:1] * first(plain[k]) + is_in[:1] * inflow[k] + is_out[:1] * va
        own[k : k + 1, :] = jnp.sum(total, 0, keepdims=True) + ghost
        send_a[k : k + 1, :] = va
        send_b[k : k + 1, :] = second(v)
    own[NK:16, :] = jnp.zeros((3, CELLS), f32)
    extra = list(params) + [rate, amp]
    for k, v in enumerate(extra):
        send_a[NK + k : NK + k + 1, :] = v[:1]
        send_b[NK + k : NK + k + 1, :] = v[:1]
        state[k : k + 1, :] = v[:1]
    send_a[23:24, :] = jnp.zeros((1, CELLS), f32)
    send_b[23:24, :] = jnp.zeros((1, CELLS), f32)
    state[10:11, :] = amp2[:1]
    state[11:16, :] = jnp.zeros((5, CELLS), f32)


NCOL = 16


def bulk_rows(params, rate, cx_a, cx_b, extra=()):
    n, ux, uy, uz, temp, qx, qy, qz = params
    inv = 1.0 / temp
    two_pi = 2.0 * np.pi * temp
    share = 1.0 / (1.0 + rate)
    scale = inv * inv / (15.0 * n)
    pref = rate * share * n * box_volume / (two_pi * jnp.sqrt(two_pi))
    rows = [uy, uz, -0.5 * inv, inv, qy * scale, qz * scale, share]
    for cx in (cx_a, cx_b):
        w = cx - ux
        square = w * w
        rows += [pref * jnp.exp(-0.5 * inv * square), qx * scale * w, square * inv]
    rows += list(extra)
    return rows + [jnp.zeros((1, CELLS), f32)] * (NCOL - len(rows))


def columns(c, base):
    return [c[:, base + j : base + j + 1] for j in range(NCOL)]


def shared_part(k, cy, cz):
    wy = cy - k[0]
    wz = cz - k[1]
    square = wy * wy + wz * wz
    return jnp.exp(square * k[2]), square * k[3] - 5.0, wy * k[4] + wz * k[5]


def relaxed(value, k, part, half):
    decay, square, heat = part
    pref, heat_x, square_x = k[7 + 3 * half : 10 + 3 * half]
    return value * k[6] + (decay * pref) * (1.0 + (heat + heat_x) * (square + square_x))


def own_kernel(ra, rb, state, wall_bulk, infl, cols, ca, cb, ghost, work):
    x, p = here()
    cxd = speed_x(p)
    sign_a = jnp.where(x % 2 == 0, 1.0, -1.0)
    cy, cz = lane_speeds(p, 16)
    st = state[...]
    rows = bulk_rows(
        [st[k : k + 1] for k in range(8)], st[8:9], sign_a * cxd, -sign_a * cxd, [st[9:10] * (courant * cxd), st[10:11]]
    )
    work[...] = to_columns(jnp.concatenate(rows, 0))

    def step(i, carry):
        at = pl.ds(pl.multiple_of(i * 16, 16), 16)
        k = columns(work[at, :], 0)
        part = shared_part(k, cy, cz)
        face = cols[at, :]
        w = wall_bulk[at, :]
        value = relaxed(ra[at, :] + k[13] * w, k, part, 0)
        ca[at, :] = value
        cb[at, :] = relaxed(rb[at, :], k, part, 1)
        ghost[at, :] = infl[at, :] * face[:, 0:1] + k[14] * w + face[:, 1:2] * value
        return carry

    lax.fori_loop(0, 16, step, 0, unroll=4)


def halo_kernel(ha, from_a, wall_bulk, pb, work):
    x, p = here()
    cxd = speed_x(p)
    cx = jnp.where(x % 2 == 0, -cxd, cxd)
    cy, cz = lane_speeds(p, 16)
    source = from_a[...]
    rows = bulk_rows(
        [source[NK + k : NK + k + 1] for k in range(8)],
        source[NK + 8 : NK + 9],
        cx,
        cx,
        [source[NK + 9 : NK + 10] * (courant * cxd)],
    )
    work[...] = to_columns(jnp.concatenate(rows, 0))

    def step(i, carry):
        at = pl.ds(pl.multiple_of(i * 16, 16), 16)
        k = columns(work[at, :], 0)
        pb[at, :] = relaxed(ha[at, :] + k[13] * wall_bulk[at, :], k, shared_part(k, cy, cz), 1)
        return carry

    lax.fori_loop(0, 16, step, 0, unroll=4)


def final_kernel(
    ca, cb, pb, ghost, hb, from_a, from_b, own, state, table, out, fields, oa, ob, work, stage, sems
):
    x, p = here()
    odd = x % 2
    cxd = speed_x(p)
    sign_a = jnp.where(odd == 0, 1.0, -1.0)
    cx_a, cx_b = sign_a * cxd, -sign_a * cxd
    cy, cz = lane_speeds(p, 16)
    weights = transport_weights(cxd, cy, cz)
    edge = jnp.where(jnp.logical_or(x == 0, x == 7), 1.0, 0.0)
    inner = 1.0 - edge
    ta, tb, st = from_a[...], from_b[...], state[...]
    m = [spread(own[k : k + 1, :] + ta[k : k + 1] + tb[k : k + 1]) for k in range(NK)]
    params, rate = relax_params(m, table[...])
    table8 = jnp.concatenate([v[:1] for v in params], 0)
    for y in range(16):
        stage[:, y, :] = table8[:, 16 * y : 16 * y + 16]
    copies = [pltpu.make_async_copy(stage, fields, sems.at[8])]
    copies[0].start()
    tb = jnp.where(edge > 0.0, st[:10], tb[NK : NK + 10])

    rows = bulk_rows([tb[k : k + 1] for k in range(8)], tb[8:9], cx_a, cx_b)
    rows += bulk_rows([v[:1] for v in params], rate[:1], cx_a, cx_b)
    work[...] = to_columns(jnp.concatenate(rows, 0))

    for chunk, (begin, end) in enumerate(((0, 5), (5, 10), (10, 14), (14, 16))):

        def second(i, carry):
            at = pl.ds(pl.multiple_of(i * 16, 16), 16)
            up = upwind_y(p, i)
            c = work[at, :]
            kb, k = columns(c, 0), columns(c, NCOL)
            part = shared_part(k, cy, cz)
            halo = relaxed(hb[at, :], kb, shared_part(kb, cy, cz), 0)
            read = transport_block(ca[at, :], ca[up, :], inner * halo + ghost[at, :], weights)
            oa[at, :] = relaxed(read, k, part, 0)
            read = transport_block(cb[at, :], cb[up, :], pb[at, :], weights)
            ob[at, :] = relaxed(read, k, part, 1)
            return carry

        lax.fori_loop(begin, end, second, 0, unroll=end - begin)
        at = pl.ds(16 * begin, 16 * (end - begin))
        for half, source, start in ((0, oa, 1 - odd), (1, ob, odd)):
            copy = pltpu.make_async_copy(
                source.at[at, :], out.at[at, pl.ds(half_start(start), HALF)], sems.at[2 * chunk + half]
            )
            copy.start()
            copies.append(copy)
    for copy in copies:
        copy.wait()


VMEM = pl.BlockSpec(memory_space=pltpu.VMEM)
ANY = pl.BlockSpec(memory_space=pltpu.HBM)
PLANE = (CELLS, HALF)
PARTS = (2 * ROWS, HALF)


def call(kernel, outs, args, scratch=(), sems=0, loose_in=(), loose_out=(), cost=1_000_000, grant=16):
    scratches = [pltpu.VMEM(s, f32) for s in scratch]
    if sems:
        scratches.append(pltpu.SemaphoreType.DMA((sems,)))
    return pl.pallas_call(
        kernel,
        out_shape=[jax.ShapeDtypeStruct(s, jnp.bfloat16 if s is PARTS else f32) for s in outs],
        in_specs=[ANY if k in loose_in else VMEM for k in range(len(args))],
        out_specs=[ANY if k in loose_out else VMEM for k in range(len(outs))],
        scratch_shapes=scratches,
        cost_estimate=pl.CostEstimate(flops=cost, bytes_accessed=1 << 20, transcendentals=0),
        compiler_params=pltpu.CompilerParams(vmem_limit_bytes=grant << 20),
    )(*args)


PAIRS_A = [(i, i ^ 1) for i in range(8)]
PAIRS_B = [pair for i in (1, 3, 5) for pair in ((i, i + 1), (i + 1, i))]
SWAP = [(0, 1), (1, 0)]


def both_ways(pairs):
    return [pair for i, j in pairs for pair in ((i, j), (j, i))]


Z_ROUNDS = [
    ("zround1", both_ways([(0, 1), (2, 3), (4, 5), (6, 7)])),
    ("zround2", both_ways([(0, 2), (1, 3), (4, 6), (5, 7)])),
    ("zround3", both_ways([(0, 6), (1, 7), (2, 4), (3, 5)])),
]


def swap_planes(a, b):
    b = lax.ppermute(b, "space", PAIRS_B)
    a = lax.ppermute(a, "space", PAIRS_A)
    return a, b


def body(distribution, inflow, wall_temp, face_type):
    f = distribution.reshape(CELLS, 2 * HALF)
    fa, fb = call(split_kernel, [PLANE, PLANE], [f], sems=2, loose_in=(0,))
    ha, hb = swap_planes(fa, fb)
    temp = wall_temp.reshape(2, CELLS)
    kind = face_type.reshape(2, CELLS)
    table = jnp.asarray(TABLE)
    infl, wa, wb, pre, wall, wall_bulk, cols = call(
        setup_kernel,
        [PLANE, PARTS, PARTS, (ROWS, CELLS), (2 * NK * 8, CELLS), PLANE, (CELLS, 128)],
        [inflow.reshape(2, CELLS, 2 * HALF), fb, temp, kind, jnp.asarray(WALL_TABLES)],
        scratch=[(ROWS, HALF)] * 2,
        sems=1,
        loose_in=(0,),
    )
    rb, rows_b = call(read_b_kernel, [PLANE, (ROWS, CELLS)], [fb, ha, wb, pre])
    ra, keep, send = call(
        read_a_kernel, [PLANE, (HROWS, CELLS), (HROWS, CELLS)], [fa, hb, infl, cols, wa, rows_b]
    )
    part = keep + lax.ppermute(send, "core", SWAP)
    part = part + lax.ppermute(part, "ylo", SWAP)
    ga = lax.optimization_barrier((ra, part))[0]
    gb = rb
    for name, pairs in Z_ROUNDS:
        if name == "zround2":
            gb = lax.optimization_barrier((rb, part))[0]
        part = part + lax.ppermute(part, "z", pairs)
    ga, gb = swap_planes(ga, gb)
    other = lax.ppermute(part, "core", SWAP)
    send_a, send_b, own, state = call(
        cell_kernel,
        [(24, CELLS), (24, CELLS), (16, CELLS), (16, CELLS)],
        [part, other, wall, kind, table],
    )
    from_a, from_b = swap_planes(send_a, send_b)
    ca, cb, ghost = call(
        own_kernel, [PLANE] * 3, [ra, rb, state, wall_bulk, infl, cols], scratch=[(CELLS, 128)]
    )
    (pb,) = call(halo_kernel, [PLANE], [ga, from_a, wall_bulk], scratch=[(CELLS, 128)])
    out, fields = call(
        final_kernel,
        [(CELLS, 2 * HALF), (8, 16, 16)],
        [ca, cb, pb, ghost, gb, from_a, from_b, own, state, table],
        scratch=[PLANE] * 2 + [(CELLS, 128), (8, 16, 16)],
        sems=9,
        loose_out=(0, 1),
    )
    return out.reshape(1, 16, 16, 2 * HALF), fields[:, None]


def solution(mesh):
    split = Mesh(mesh.devices.reshape(8, 8, 2, 2), ("space", "z", "ylo", "core"))
    vel = ("z", "ylo", "core")
    in_specs = (P("space", None, None, vel), P(None, None, None, vel), P(), P())
    out_specs = (P("space", None, None, vel), P(None, "space", None, None))

    return jax.shard_map(body, mesh=split, in_specs=in_specs, out_specs=out_specs, check_vma=False)
```

```python
import jax
import jax.numpy as jnp
import numpy as np
from jax import lax
from jax.experimental import pallas as pl
from jax.experimental.pallas import tpu as pltpu
from jax.sharding import Mesh, PartitionSpec as P


NV = 32768
CELLS = 256
HALF = 512
NK = 13
ROWS = 96
HROWS = ROWS // 2
courant = 0.08
rate_field = 0.8
box_volume = 512.0
HIGHEST = lax.Precision.HIGHEST
f32 = jnp.float32

MOMENTS = [
    [(0, 0, 0)],
    [(1, 0, 0)],
    [(0, 1, 0)],
    [(0, 0, 1)],
    [(2, 0, 0)],
    [(0, 2, 0)],
    [(0, 0, 2)],
    [(1, 1, 0)],
    [(1, 0, 1)],
    [(0, 1, 1)],
    [(3, 0, 0), (1, 2, 0), (1, 0, 2)],
    [(2, 1, 0), (0, 3, 0), (0, 1, 2)],
    [(2, 0, 1), (0, 2, 1), (0, 0, 3)],
]


def axis_table(top):
    grid = (np.arange(32) + 0.5) * 0.25 - 4.0
    plus, minus = courant * np.maximum(grid, 0.0), courant * np.maximum(-grid, 0.0)
    table = np.zeros((24 * top, 96))
    for axis in range(3):
        for power in range(top):
            for d in range(7):
                row = grid**power
                if d == 1 + 2 * axis:
                    row = row * plus
                if d == 2 + 2 * axis:
                    row = row * minus
                table[8 * top * axis + 8 * power + d, 32 * axis : 32 * axis + 32] = row
    return table.astype(np.float32), plus, minus


def wall_tables():
    table, plus, minus = axis_table(4)
    walls = []
    for weight in (plus, minus):
        wall = table.copy()
        wall[:32, :32] *= weight
        walls.append(np.concatenate([table, wall]))
    return np.stack(walls).astype(np.float32)


TOP = 5


def two_parts(table):
    table = np.concatenate([table, np.zeros((-len(table) % 16, 96), np.float32)])
    high = table.astype(jnp.bfloat16)
    low = (table - high.astype(np.float32)).astype(jnp.bfloat16)
    return np.concatenate([high, low])


TABLE = two_parts(axis_table(TOP)[0])
WALL_TABLES = wall_tables()


def dot(a, b):
    return lax.dot_general(a, b, (((1,), (0,)), ((), ())), precision=HIGHEST, preferred_element_type=f32)


def dot_t(a, b):
    return lax.dot_general(a, b, (((1,), (1,)), ((), ())), precision=HIGHEST, preferred_element_type=f32)


def split(a):
    high = a.astype(jnp.bfloat16)
    return high, (a - high.astype(f32)).astype(jnp.bfloat16)


def dot_parts(parts, b, side):
    high, low = split(b)
    rows = parts.shape[0] // 2
    dims = (((1,), (side,)), ((), ()))
    first = lax.dot_general(parts, high, dims, preferred_element_type=f32)
    second = lax.dot_general(parts, low, dims, preferred_element_type=f32)
    return first[:rows] + (first[rows:] + second[:rows] + second[rows:])


def tile4(a):
    return jnp.concatenate([a] * 4, 0)


def speed_grid():
    return (lax.broadcasted_iota(jnp.int32, (32, CELLS), 0).astype(f32) + 0.5) * 0.25 - 4.0


def lane_speeds(p, rows):
    lane = lax.broadcasted_iota(jnp.int32, (rows, HALF), 1)
    cy = ((lane // 32 + (p % 2) * 16).astype(f32) + 0.5) * 0.25 - 4.0
    cz = ((lane % 32).astype(f32) + 0.5) * 0.25 - 4.0
    return cy, cz


def speed_x(p):
    return ((p // 2).astype(f32) + 0.5) * 0.25


def to_columns(rows):
    pad = 128 - rows.shape[0]
    return jnp.transpose(jnp.concatenate([rows, jnp.zeros((pad, CELLS), f32)], 0))


def equilibrium_moments(params, table):
    n, ux, uy, uz, temp, qx, qy, qz = params
    inv = 1.0 / temp
    two_pi = 2.0 * np.pi * temp
    pref = n * box_volume / (two_pi * jnp.sqrt(two_pi))
    scale = inv * inv / (15.0 * n)
    grid = speed_grid()
    decay = tile4(-0.5 * inv)
    columns = []
    for u in (ux, uy, uz):
        w = grid - tile4(u)
        square = w * w
        g = jnp.exp(square * decay)
        columns.append(jnp.concatenate([g, g * square], 1))
    sums = dot_parts(table, jnp.concatenate(columns, 0), 0)
    factors = []
    for axis, (u, q) in enumerate(((ux, qx), (uy, qy), (uz, qz))):
        kq = q * scale
        starts = [8 * (TOP * axis + power) for power in range(TOP)]
        even0 = [sums[row : row + 8, :CELLS] for row in starts]
        even2 = [sums[row : row + 8, CELLS:] for row in starts]
        powers = []
        for power in range(4):
            t0, t2 = even0[power], even2[power]
            t1 = even0[power + 1] - u * t0
            t3 = even2[power + 1] - u * t2
            powers.append((t0, kq * t1, t2 * inv, kq * (t3 * inv - 5.0 * t1)))
        factors.append(powers)
    xs, ys, zs = factors
    pairs = {}

    def pair(ay, az):
        if (ay, az) not in pairs:
            y0, y1, y2, y3 = ys[ay]
            z0, z1, z2, z3 = zs[az]
            a = y0 * z0
            b = a + y3 * z0 + y0 * z3 + y1 * z2 + y2 * z1
            pairs[(ay, az)] = (a, b, y2 * z0 + y0 * z2, y1 * z0 + y0 * z1)
        return pairs[(ay, az)]

    out = []
    for terms in MOMENTS:
        total = 0.0
        for ax, ay, az in terms:
            x0, x1, x2, x3 = xs[ax]
            a, b, c, d = pair(ay, az)
            total = total + (x0 * b + x3 * a + x1 * c + x2 * d)
        out.append(pref * total)
    return out


def wall_moments(temp, tables):
    grid = speed_grid()
    g = jnp.exp(grid * grid * tile4(-0.5 / temp))
    sums = dot(tables, jnp.concatenate([g] * 3, 0))
    two_pi = 2.0 * np.pi * temp
    pref = box_volume / (two_pi * jnp.sqrt(two_pi))
    out = []
    for base in (0, 96):
        for terms in MOMENTS:
            total = 0.0
            for powers in terms:
                part = pref
                for axis in range(3):
                    row = base + 32 * axis + 8 * powers[axis]
                    part = part * sums[row : row + 8]
                total = total + part
            out.append(total)
    return out


def macro(m):
    m = [a * (1.0 / NV) for a in m]
    n = m[0]
    rn = 1.0 / n
    ux, uy, uz = m[1] * rn, m[2] * rn, m[3] * rn
    square = ux * ux + uy * uy + uz * uz
    energy = m[4] + m[5] + m[6]
    temp = (energy - n * square) * rn * (1.0 / 3.0)
    lift = 2.0 * n * square - energy
    qx = 0.5 * (m[10] + ux * lift) - (ux * m[4] + uy * m[7] + uz * m[8])
    qy = 0.5 * (m[11] + uy * lift) - (ux * m[7] + uy * m[5] + uz * m[9])
    qz = 0.5 * (m[12] + uz * lift) - (ux * m[8] + uy * m[9] + uz * m[6])
    rate = rate_field * n * jnp.exp(0.19 * jnp.log(temp))
    return (n, ux, uy, uz, temp, qx, qy, qz), rate


def spread(row):
    return jnp.broadcast_to(row, (8, CELLS))


def relax_params(m, table):
    params, rate = macro(m)
    for _ in range(2):
        s = [spread(a[:1]) for a in equilibrium_moments(params, table)]
        inv = 1.0 / (1.0 + rate)
        params, rate = macro([(a + rate * b) * inv for a, b in zip(m, s)])
    return params, rate


def here():
    x = lax.axis_index("space")
    p = lax.axis_index("z") * 4 + lax.axis_index("ylo") * 2 + lax.axis_index("core")
    return x, p


def half_start(index):
    return pl.multiple_of(index * HALF, HALF)


def split_kernel(f, fa, fb, sems):
    x, _ = here()
    odd = x % 2
    first = pltpu.make_async_copy(f.at[:, pl.ds(half_start(1 - odd), HALF)], fa, sems.at[0])
    second = pltpu.make_async_copy(f.at[:, pl.ds(half_start(odd), HALF)], fb, sems.at[1])
    first.start()
    second.start()
    first.wait()
    second.wait()


def setup_kernel(inflow, fb, temp_ref, type_ref, tables, infl, pa, pb, pre, wall, wall_bulk, cols, wa, wb, sems):
    x, p = here()
    odd = x % 2
    face = jnp.where(x >= 4, 1, 0)
    copy = pltpu.make_async_copy(inflow.at[face, :, pl.ds(half_start(1 - odd), HALF)], infl, sems.at[0])
    copy.start()
    cxd = speed_x(p)
    cy, cz = lane_speeds(p, 8)
    d = lax.broadcasted_iota(jnp.int32, (8, HALF), 0)
    yp, ym = courant * jnp.maximum(cy, 0.0), courant * jnp.maximum(-cy, 0.0)
    zp, zm = courant * jnp.maximum(cz, 0.0), courant * jnp.maximum(-cz, 0.0)
    sign_a = jnp.where(odd == 0, 1.0, -1.0)
    for w, sign in ((wa, sign_a), (wb, -sign_a)):
        cx = sign * cxd
        xp, xm = courant * jnp.maximum(cx, 0.0), courant * jnp.maximum(-cx, 0.0)
        plus = jnp.where(d == 0, 1.0, jnp.where(d == 1, xp, jnp.where(d == 3, yp, jnp.where(d == 5, zp, 0.0))))
        full = jnp.where(d == 2, xm, jnp.where(d == 4, ym, jnp.where(d == 6, zm, plus)))
        ypow = [1.0, cy, cy * cy, cy * cy * cy]
        zpow = [1.0, cz, cz * cz, cz * cz * cz]
        xpow = [1.0, cx, cx * cx, cx * cx * cx]
        phis = []
        for terms in MOMENTS:
            phi = 0.0
            for ax, ay, az in terms:
                phi = phi + xpow[ax] * (ypow[ay] * zpow[az])
            phis.append(phi)
        gaps = jnp.where(d == 2, xp, jnp.where(d == 4, yp, jnp.where(d == 6, zp, 0.0)))
        w[0:8, :] = plus * phis[0] + gaps * phis[3]
        w[8:16, :] = plus * phis[1] + jnp.where(d == 2, phis[3], 0.0)
        w[16:24, :] = plus * phis[2]
        for k in range(4, NK):
            w[8 * k - 8 : 8 * k, :] = full * phis[k]
    edge = jnp.where(jnp.logical_or(x == 0, x == 7), 1.0, 0.0)
    sub = lax.broadcasted_iota(jnp.int32, (8, CELLS), 0)
    temp = jnp.broadcast_to(temp_ref[pl.ds(face, 1), :], (8, CELLS))
    kind = jnp.broadcast_to(type_ref[pl.ds(face, 1), :], (8, CELLS))
    for k, value in enumerate(wall_moments(temp, tables[face])):
        wall[8 * k : 8 * k + 8, :] = value
    two_pi = 2.0 * np.pi * temp
    rows = jnp.where(sub == 0, jnp.where(kind == 1, edge, 0.0), 0.0)
    rows = jnp.where(sub == 1, jnp.where(kind == 2, edge, 0.0), rows)
    rows = jnp.where(sub == 2, -0.5 / temp, rows)
    rows = jnp.where(sub == 3, box_volume / (two_pi * jnp.sqrt(two_pi)), rows)
    cols[...] = to_columns(rows)
    cy16, cz16 = lane_speeds(p, 16)
    speed_sq = cy16 * cy16 + cz16 * cz16 + cxd * cxd

    def step(i, carry):
        at = pl.ds(pl.multiple_of(i * 16, 16), 16)
        c = cols[at, :]
        wall_bulk[at, :] = c[:, 3:4] * jnp.exp(speed_sq * c[:, 2:3])
        return carry

    lax.fori_loop(0, 16, step, 0, unroll=8)
    for w, parts in ((wa, pa), (wb, pb)):
        high, low = split(w[...])
        parts[:ROWS, :] = high
        parts[ROWS:, :] = low
    flux = dot_t(jnp.full((8, HALF), 1.0, f32), fb[...]) * (cxd * edge)
    copy.wait()
    in_rows = dot_t(wa[...], infl[...]) * (courant * cxd * edge)
    for group in range(ROWS // 8):
        value = jnp.where(sub == 7, spread(in_rows[8 * group : 8 * group + 1]), 0.0)
        if group == 1:
            value = jnp.where(sub == 6, spread(in_rows[10:11]), jnp.where(sub == 4, flux, value))
        pre[8 * group : 8 * group + 8, :] = value


def upwind_y(p, i):
    return pl.ds(pl.multiple_of(((i + jnp.where(p % 2 == 1, 15, 1)) % 16) * 16, 16), 16)


def transport_weights(cxd, cy, cz):
    abs_y, abs_z = courant * jnp.abs(cy), courant * jnp.abs(cz)
    return 1.0 - courant * cxd - abs_y - abs_z, courant * cxd, abs_y, abs_z, cz > 0.0


def transport_block(value, neighbour_y, plane, weights):
    centre, abs_x, abs_y, abs_z, forward = weights
    neighbour_z = jnp.where(forward, pltpu.roll(value, 1, 0), pltpu.roll(value, 15, 0))
    return value * centre + abs_x * plane + abs_y * neighbour_y + abs_z * neighbour_z


def read_b_kernel(fb, ha, wb, pre, rb, rows):
    _, p = here()
    weights = transport_weights(speed_x(p), *lane_speeds(p, 16))

    def step(i, carry):
        at = pl.ds(pl.multiple_of(i * 16, 16), 16)
        rb[at, :] = transport_block(fb[at, :], fb[upwind_y(p, i), :], ha[at, :], weights)
        return carry

    lax.fori_loop(0, 16, step, 0, unroll=8)
    rows[...] = pre[...] + dot_parts(wb[...], rb[...], 1)


def read_a_kernel(fa, hb, infl, cols, wa, rows_b, ra, keep, send):
    x, p = here()
    inner = jnp.where(jnp.logical_or(x == 0, x == 7), 0.0, 1.0)
    weights = transport_weights(speed_x(p), *lane_speeds(p, 16))

    def step(i, carry):
        at = pl.ds(pl.multiple_of(i * 16, 16), 16)
        c = cols[at, :]
        value = fa[at, :]
        plane = hb[at, :] * inner + infl[at, :] * c[:, 0:1] + c[:, 1:2] * value
        ra[at, :] = transport_block(value, fa[upwind_y(p, i), :], plane, weights)
        return carry

    lax.fori_loop(0, 16, step, 0, unroll=8)
    rows = rows_b[...] + dot_parts(wa[...], ra[...], 1)
    north = p % 2 == 1
    top, bottom = rows[:HROWS], rows[HROWS:]
    keep[...] = jnp.where(north, bottom, top)
    send[...] = jnp.where(north, top, bottom)


def unpack_rows(groups, sub):
    first, second = groups[0], groups[1]
    plain = [groups[0][:1], groups[1][:1], groups[2][:1], groups[1][2:3]] + [g[:1] for g in groups[3:]]
    odd = jnp.logical_or(sub == 1, jnp.logical_or(sub == 3, sub == 5))
    even = jnp.logical_or(sub == 2, jnp.logical_or(sub == 4, sub == 6))
    products = [(1, 2, 3), (4, 7, 8), (7, 5, 9), (8, 9, 6)]

    def less(plus, k):
        ix, iy, iz = products[k]
        change = jnp.where(sub == 2, spread(plain[ix]), jnp.where(sub == 4, spread(plain[iy]), spread(plain[iz])))
        return plus - courant * change

    out = []
    for k in range(3):
        out.append(jnp.where(even, less(pltpu.roll(groups[k], 1, 0), k), groups[k]))
    rest = jnp.where(sub == 0, spread(second[2:3]), spread(second[6:7]))
    out.append(jnp.where(odd, pltpu.roll(first, 7, 0), jnp.where(even, less(first, 3), rest)))
    return out + list(groups[3:]), second[4:5]


def cell_kernel(mine, other, wall, type_ref, table, send_a, send_b, own, state):
    x, p = here()
    upper = x == 7
    odd = x % 2 == 1
    face = jnp.where(x >= 4, 1, 0)
    edge = jnp.where(jnp.logical_or(x == 0, upper), 1.0, 0.0)
    north = p % 2 == 1
    a, b = mine[...], other[...]
    rows = jnp.concatenate([jnp.where(north, b, a), jnp.where(north, a, b)], 0)
    sub = lax.broadcasted_iota(jnp.int32, (8, CELLS), 0)
    m, leaving = unpack_rows([rows[8 * k : 8 * k + 8] for k in range(ROWS // 8)], sub)
    plain = [wall[8 * k : 8 * k + 8, :] for k in range(NK)]
    kind = jnp.broadcast_to(type_ref[pl.ds(face, 1), :], (8, CELLS))
    is_wall = jnp.where(kind == 0, edge, 0.0)
    is_in = jnp.where(kind == 1, edge, 0.0)
    is_out = jnp.where(kind == 2, edge, 0.0)

    def first(v):
        return jnp.where(odd, v[2:3], v[1:2])

    def second(v):
        return jnp.where(odd, v[1:2], v[2:3])

    entering = spread(first(plain[0])) * (1.0 / courant)
    amp = is_wall * spread(leaving) / entering
    inflow = [v[7:8] for v in m]
    m = [v + amp * wall[8 * (NK + k) : 8 * (NK + k) + 8, :] for k, v in enumerate(m)]
    params, rate = relax_params([spread(v[:1]) for v in m], table[...])
    s = equilibrium_moments(params, table[...])
    inv = 1.0 / (1.0 + rate)
    m = [(v + rate * w) * inv for v, w in zip(m, s)]
    amp2 = is_wall * spread(second(m[0])) * (1.0 / courant) / entering
    lane = lax.broadcasted_iota(jnp.int32, (8, CELLS), 1)
    low, high = lane % 16 == 0, lane % 16 == 15
    for k in range(NK):
        v = m[k]
        z_up = jnp.where(low, pltpu.roll(v, CELLS - 15, 1), pltpu.roll(v, 1, 1))
        z_down = jnp.where(high, pltpu.roll(v, 15, 1), pltpu.roll(v, CELLS - 1, 1))
        total = jnp.where(sub == 0, v, jnp.where(sub == 7, 0.0, -v))
        total = total + jnp.where(sub == 3, pltpu.roll(v, 16, 1), 0.0)
        total = total + jnp.where(sub == 4, pltpu.roll(v, CELLS - 16, 1), 0.0)
        total = total + jnp.where(sub == 5, z_up, 0.0) + jnp.where(sub == 6, z_down, 0.0)
        va = first(v)
        ghost = amp2[:1] * first(plain[k]) + is_in[:1] * inflow[k] + is_out[:1] * va
        own[k : k + 1, :] = jnp.sum(total, 0, keepdims=True) + ghost
        send_a[k : k + 1, :] = va
        send_b[k : k + 1, :] = second(v)
    own[NK:16, :] = jnp.zeros((3, CELLS), f32)
    extra = list(params) + [rate, amp]
    for k, v in enumerate(extra):
        send_a[NK + k : NK + k + 1, :] = v[:1]
        send_b[NK + k : NK + k + 1, :] = v[:1]
        state[k : k + 1, :] = v[:1]
    send_a[23:24, :] = jnp.zeros((1, CELLS), f32)
    send_b[23:24, :] = jnp.zeros((1, CELLS), f32)
    state[10:11, :] = amp2[:1]
    state[11:16, :] = jnp.zeros((5, CELLS), f32)


NCOL = 16


def bulk_rows(params, rate, cx_a, cx_b, extra=()):
    n, ux, uy, uz, temp, qx, qy, qz = params
    inv = 1.0 / temp
    two_pi = 2.0 * np.pi * temp
    share = 1.0 / (1.0 + rate)
    scale = inv * inv / (15.0 * n)
    pref = rate * share * n * box_volume / (two_pi * jnp.sqrt(two_pi))
    rows = [uy, uz, -0.5 * inv, inv, qy * scale, qz * scale, share]
    for cx in (cx_a, cx_b):
        w = cx - ux
        square = w * w
        rows += [pref * jnp.exp(-0.5 * inv * square), qx * scale * w, square * inv]
    rows += list(extra)
    return rows + [jnp.zeros((1, CELLS), f32)] * (NCOL - len(rows))


def columns(c, base):
    return [c[:, base + j : base + j + 1] for j in range(NCOL)]


def shared_part(k, cy, cz):
    wy = cy - k[0]
    wz = cz - k[1]
    square = wy * wy + wz * wz
    return jnp.exp(square * k[2]), square * k[3] - 5.0, wy * k[4] + wz * k[5]


def relaxed(value, k, part, half):
    decay, square, heat = part
    pref, heat_x, square_x = k[7 + 3 * half : 10 + 3 * half]
    return value * k[6] + (decay * pref) * (1.0 + (heat + heat_x) * (square + square_x))


def own_kernel(ra, rb, state, wall_bulk, infl, cols, ca, cb, ghost, work):
    x, p = here()
    cxd = speed_x(p)
    sign_a = jnp.where(x % 2 == 0, 1.0, -1.0)
    cy, cz = lane_speeds(p, 16)
    st = state[...]
    rows = bulk_rows(
        [st[k : k + 1] for k in range(8)], st[8:9], sign_a * cxd, -sign_a * cxd, [st[9:10] * (courant * cxd), st[10:11]]
    )
    work[...] = to_columns(jnp.concatenate(rows, 0))

    def step(i, carry):
        at = pl.ds(pl.multiple_of(i * 16, 16), 16)
        k = columns(work[at, :], 0)
        part = shared_part(k, cy, cz)
        face = cols[at, :]
        w = wall_bulk[at, :]
        value = relaxed(ra[at, :] + k[13] * w, k, part, 0)
        ca[at, :] = value
        cb[at, :] = relaxed(rb[at, :], k, part, 1)
        ghost[at, :] = infl[at, :] * face[:, 0:1] + k[14] * w + face[:, 1:2] * value
        return carry

    lax.fori_loop(0, 16, step, 0, unroll=8)


def halo_kernel(ha, from_a, wall_bulk, pb, work):
    x, p = here()
    cxd = speed_x(p)
    cx = jnp.where(x % 2 == 0, -cxd, cxd)
    cy, cz = lane_speeds(p, 16)
    source = from_a[...]
    rows = bulk_rows(
        [source[NK + k : NK + k + 1] for k in range(8)],
        source[NK + 8 : NK + 9],
        cx,
        cx,
        [source[NK + 9 : NK + 10] * (courant * cxd)],
    )
    work[...] = to_columns(jnp.concatenate(rows, 0))

    def step(i, carry):
        at = pl.ds(pl.multiple_of(i * 16, 16), 16)
        k = columns(work[at, :], 0)
        pb[at, :] = relaxed(ha[at, :] + k[13] * wall_bulk[at, :], k, shared_part(k, cy, cz), 1)
        return carry

    lax.fori_loop(0, 16, step, 0, unroll=8)


def final_kernel(
    ca, cb, pb, ghost, hb, from_a, from_b, own, state, table, out, fields, oa, ob, work, stage, sems
):
    x, p = here()
    odd = x % 2
    cxd = speed_x(p)
    sign_a = jnp.where(odd == 0, 1.0, -1.0)
    cx_a, cx_b = sign_a * cxd, -sign_a * cxd
    cy, cz = lane_speeds(p, 16)
    weights = transport_weights(cxd, cy, cz)
    edge = jnp.where(jnp.logical_or(x == 0, x == 7), 1.0, 0.0)
    inner = 1.0 - edge
    ta, tb, st = from_a[...], from_b[...], state[...]
    m = [spread(own[k : k + 1, :] + ta[k : k + 1] + tb[k : k + 1]) for k in range(NK)]
    params, rate = relax_params(m, table[...])
    table8 = jnp.concatenate([v[:1] for v in params], 0)
    for y in range(16):
        stage[:, y, :] = table8[:, 16 * y : 16 * y + 16]
    copies = [pltpu.make_async_copy(stage, fields, sems.at[8])]
    copies[0].start()
    tb = jnp.where(edge > 0.0, st[:10], tb[NK : NK + 10])

    rows = bulk_rows([tb[k : k + 1] for k in range(8)], tb[8:9], cx_a, cx_b)
    rows += bulk_rows([v[:1] for v in params], rate[:1], cx_a, cx_b)
    work[...] = to_columns(jnp.concatenate(rows, 0))

    for chunk, (begin, end) in enumerate(((0, 5), (5, 10), (10, 14), (14, 16))):

        def second(i, carry):
            at = pl.ds(pl.multiple_of(i * 16, 16), 16)
            up = upwind_y(p, i)
            c = work[at, :]
            kb, k = columns(c, 0), columns(c, NCOL)
            part = shared_part(k, cy, cz)
            halo = relaxed(hb[at, :], kb, shared_part(kb, cy, cz), 0)
            read = transport_block(ca[at, :], ca[up, :], inner * halo + ghost[at, :], weights)
            oa[at, :] = relaxed(read, k, part, 0)
            read = transport_block(cb[at, :], cb[up, :], pb[at, :], weights)
            ob[at, :] = relaxed(read, k, part, 1)
            return carry

        lax.fori_loop(begin, end, second, 0, unroll=end - begin)
        at = pl.ds(16 * begin, 16 * (end - begin))
        for half, source, start in ((0, oa, 1 - odd), (1, ob, odd)):
            copy = pltpu.make_async_copy(
                source.at[at, :], out.at[at, pl.ds(half_start(start), HALF)], sems.at[2 * chunk + half]
            )
            copy.start()
            copies.append(copy)
    for copy in copies:
        copy.wait()


VMEM = pl.BlockSpec(memory_space=pltpu.VMEM)
ANY = pl.BlockSpec(memory_space=pltpu.HBM)
PLANE = (CELLS, HALF)
PARTS = (2 * ROWS, HALF)


def call(kernel, outs, args, scratch=(), sems=0, loose_in=(), loose_out=(), cost=1_000_000, grant=16):
    scratches = [pltpu.VMEM(s, f32) for s in scratch]
    if sems:
        scratches.append(pltpu.SemaphoreType.DMA((sems,)))
    return pl.pallas_call(
        kernel,
        out_shape=[jax.ShapeDtypeStruct(s, jnp.bfloat16 if s is PARTS else f32) for s in outs],
        in_specs=[ANY if k in loose_in else VMEM for k in range(len(args))],
        out_specs=[ANY if k in loose_out else VMEM for k in range(len(outs))],
        scratch_shapes=scratches,
        cost_estimate=pl.CostEstimate(flops=cost, bytes_accessed=1 << 20, transcendentals=0),
        compiler_params=pltpu.CompilerParams(vmem_limit_bytes=grant << 20),
    )(*args)


PAIRS_A = [(i, i ^ 1) for i in range(8)]
PAIRS_B = [pair for i in (1, 3, 5) for pair in ((i, i + 1), (i + 1, i))]
SWAP = [(0, 1), (1, 0)]


def both_ways(pairs):
    return [pair for i, j in pairs for pair in ((i, j), (j, i))]


Z_ROUNDS = [
    ("zround1", both_ways([(0, 1), (2, 3), (4, 5), (6, 7)])),
    ("zround2", both_ways([(0, 2), (1, 3), (4, 6), (5, 7)])),
    ("zround3", both_ways([(0, 6), (1, 7), (2, 4), (3, 5)])),
]


def swap_planes(a, b):
    b = lax.ppermute(b, "space", PAIRS_B)
    a = lax.ppermute(a, "space", PAIRS_A)
    return a, b


def body(distribution, inflow, wall_temp, face_type):
    f = distribution.reshape(CELLS, 2 * HALF)
    fa, fb = call(split_kernel, [PLANE, PLANE], [f], sems=2, loose_in=(0,))
    ha, hb = swap_planes(fa, fb)
    temp = wall_temp.reshape(2, CELLS)
    kind = face_type.reshape(2, CELLS)
    table = jnp.asarray(TABLE)
    infl, wa, wb, pre, wall, wall_bulk, cols = call(
        setup_kernel,
        [PLANE, PARTS, PARTS, (ROWS, CELLS), (2 * NK * 8, CELLS), PLANE, (CELLS, 128)],
        [inflow.reshape(2, CELLS, 2 * HALF), fb, temp, kind, jnp.asarray(WALL_TABLES)],
        scratch=[(ROWS, HALF)] * 2,
        sems=1,
        loose_in=(0,),
    )
    rb, rows_b = call(read_b_kernel, [PLANE, (ROWS, CELLS)], [fb, ha, wb, pre])
    ra, keep, send = call(
        read_a_kernel, [PLANE, (HROWS, CELLS), (HROWS, CELLS)], [fa, hb, infl, cols, wa, rows_b]
    )
    part = keep + lax.ppermute(send, "core", SWAP)
    part = part + lax.ppermute(part, "ylo", SWAP)
    ga = lax.optimization_barrier((ra, part))[0]
    gb = rb
    for name, pairs in Z_ROUNDS:
        if name == "zround2":
            gb = lax.optimization_barrier((rb, part))[0]
        part = part + lax.ppermute(part, "z", pairs)
    ga, gb = swap_planes(ga, gb)
    other = lax.ppermute(part, "core", SWAP)
    send_a, send_b, own, state = call(
        cell_kernel,
        [(24, CELLS), (24, CELLS), (16, CELLS), (16, CELLS)],
        [part, other, wall, kind, table],
    )
    from_a, from_b = swap_planes(send_a, send_b)
    ca, cb, ghost = call(
        own_kernel, [PLANE] * 3, [ra, rb, state, wall_bulk, infl, cols], scratch=[(CELLS, 128)]
    )
    (pb,) = call(halo_kernel, [PLANE], [ga, from_a, wall_bulk], scratch=[(CELLS, 128)])
    out, fields = call(
        final_kernel,
        [(CELLS, 2 * HALF), (8, 16, 16)],
        [ca, cb, pb, ghost, gb, from_a, from_b, own, state, table],
        scratch=[PLANE] * 2 + [(CELLS, 128), (8, 16, 16)],
        sems=9,
        loose_out=(0, 1),
    )
    return out.reshape(1, 16, 16, 2 * HALF), fields[:, None]


def solution(mesh):
    split = Mesh(mesh.devices.reshape(8, 8, 2, 2), ("space", "z", "ylo", "core"))
    vel = ("z", "ylo", "core")
    in_specs = (P("space", None, None, vel), P(None, None, None, vel), P(), P())
    out_specs = (P("space", None, None, vel), P(None, "space", None, None))

    return jax.shard_map(body, mesh=split, in_specs=in_specs, out_specs=out_specs, check_vma=False)
```
